256 devices in a mesh: group: 2 (over y_hi), dev: 128 (over y_lo, x, z, core).
Axes of the slice: x: 4, y: 4 (y_hi: 2, y_lo: 2; y = y_hi * 2 + y_lo), z: 8, core: 2. Of those that a mesh axis runs over, the one named last changes fastest.
Arguments:
- forces: float32 [3, 524288], P(None, ('group', 'dev')), may hold values from -4 to 4
- stencil_start: int32 [3, 524288], P(None, ('group', 'dev')), may hold values from 0 to 1023, as said below
- fraction: float32 [3, 524288], P(None, ('group', 'dev')), may hold values from 0 to 1
- tile_pairs: int32 [12288, 2], P(('group', 'dev')), may hold values from 0 to 15, as said below
- pair_count: int32 [256], P(('group', 'dev')), may hold values from 1 to 48, as said below
Outputs:
- velocity: float32 [3, 524288], P(None, ('group', 'dev'))
The draws below stay inside these ranges and needn't reach their ends.
Inputs may be any that keep to these rules, and one draw needn't show every extreme that they name: `stencil_start`: along the first dimension, a point of block b = p // 2048 starts in planes b * 4 to (b + 1) * 4 - 1; along the others it lies in 0 to 127 and 0 to 127. `tile_pairs`: tile numbers are local to the device's block of 2048 points. `pair_count`: the live slots are the first ones of each device's list; some device has all 48 live.
All inputs are finite; a program needn't handle non-finite values.
Results may differ from the reference program's by a relative error of at most 0.0003.
Values sent between devices are 32-bit elements; how exact they have to be, the bound alone decides.
A program may use at most 64 MiB of HBM per device.

```python
import jax
import jax.numpy as jnp
from jax import lax

NX = 1024
NY = 128
NZ = 128
PD = 2048
TL = 48
PX = 4
NPTS = 524288
NTILES = 4096


def draw_forces(key, part):
    subkeys = jax.random.split(jax.random.fold_in(key, 5), 1)
    base = jax.random.normal(subkeys[0], (3, NTILES, 128), jnp.float32)
    centred = base - jnp.mean(base, axis=2, keepdims=True)
    largest = jnp.max(jnp.abs(centred), axis=2, keepdims=True)
    return (4.0 * centred / largest).reshape(3, NPTS).astype(jnp.float32)


def draw_stencil_start(key, part):
    subkeys = jax.random.split(jax.random.fold_in(key, 11), 7)
    blocks = NPTS // PD
    position = jnp.arange(NPTS, dtype=jnp.int32)
    owner_block = position // PD
    tile_of = position // 128
    along_x = owner_block * PX + jax.random.randint(subkeys[0], (NPTS,), 0, PX)
    base_y = jax.random.randint(subkeys[1], (blocks,), 0, NY)[owner_block]
    tile_y = jax.random.randint(subkeys[2], (NTILES,), 0, 12)[tile_of]
    point_y = jax.random.randint(subkeys[3], (NPTS,), 0, 8)
    base_z = jax.random.randint(subkeys[4], (blocks,), 0, NZ)[owner_block]
    tile_z = jax.random.randint(subkeys[5], (NTILES,), 0, 12)[tile_of]
    point_z = jax.random.randint(subkeys[6], (NPTS,), 0, 8)
    across_y = (base_y + tile_y + point_y) % NY
    across_z = (base_z + tile_z + point_z) % NZ
    return jnp.stack([along_x, across_y, across_z]).astype(jnp.int32)


def draw_tile_pairs(key, part):
    blocks = NPTS // PD
    return jax.random.randint(jax.random.fold_in(key, 17), (blocks * TL, 2), 0, PD // 128).astype(jnp.int32)


def draw_pair_count(key, part):
    subkeys = jax.random.split(jax.random.fold_in(key, 23), 3)
    blocks = NPTS // PD
    first_draw = jax.random.randint(subkeys[0], (blocks,), 1, TL + 1)
    second_draw = jax.random.randint(subkeys[1], (blocks,), 1, TL + 1)
    counts = jnp.minimum(first_draw, second_draw)
    fullest = jax.random.randint(subkeys[2], (), 0, blocks)
    return jnp.where(jnp.arange(blocks, dtype=jnp.int32) == fullest, TL, counts).astype(jnp.int32)


def block_scale(stream_key, dims, cuts, low, high):
    loudness = 1.0
    for dim, shards_of in cuts:
        draws = jax.random.uniform(jax.random.fold_in(jax.random.fold_in(stream_key, 6), dim), (shards_of,), jnp.float32, low / len(cuts), high / len(cuts))
        loudness = loudness * jnp.repeat(jnp.exp(draws), dims[dim] // shards_of).reshape((-1,) + (1,) * (len(dims) - 1 - dim))
    return loudness


def setup_inputs(seed: int = 0) -> dict:
    keys = jax.random.split(jax.random.key(seed), 6)
    forces = draw_forces(jax.random.fold_in(keys[5], 71), 0)
    stencil_start = draw_stencil_start(jax.random.fold_in(keys[5], 71), 0)
    fraction = jnp.clip(1.0 * jax.random.uniform(keys[2], (3, NPTS), jnp.float32) ** block_scale(keys[2], (3, NPTS), ((1, 256),), -0.2, 0.2), 0.0, 1.0)
    tile_pairs = draw_tile_pairs(jax.random.fold_in(keys[5], 71), 0)
    pair_count = draw_pair_count(jax.random.fold_in(keys[5], 71), 0)
    return dict(forces=forces, stencil_start=stencil_start, fraction=fraction, tile_pairs=tile_pairs, pair_count=pair_count)


TWO_PI = 6.283185307179586
EPS_SQ = 1.0
RANGE_SQ = 16.0
NEAR_SCALE = 0.25

def spline_weights(fraction):
    square = fraction * fraction
    cube = square * fraction
    return [(1.0 - fraction) ** 3 / 6.0, (3.0 * cube - 6.0 * square + 4.0) / 6.0, (-3.0 * cube + 3.0 * square + 3.0 * fraction + 1.0) / 6.0, cube / 6.0]

def wave_numbers(index, length):
    signed_index = jnp.where(index > length // 2, index - length, index)
    return (signed_index.astype(jnp.float32) * (TWO_PI / length), index != length // 2)

def wrap_gap(gap, length):
    gap = jnp.where(gap > length // 2, gap - length, gap)
    return jnp.where(gap < -(length // 2), gap + length, gap)

def pair_terms(stencil_start, fraction, forces, pairs, count):
    tiles = stencil_start.shape[1] // 128
    slots = pairs.shape[0]
    start_tiles = stencil_start.reshape(3, tiles, 128)
    frac_tiles = fraction.reshape(3, tiles, 128)
    force_tiles = forces.reshape(3, tiles, 128)
    target = pairs[:, 0]
    source = pairs[:, 1]
    lengths = (NX, NY, NZ)
    deltas = []
    for component in range(3):
        gap = start_tiles[component][target][:, :, None] - start_tiles[component][source][:, None, :]
        if component > 0:
            gap = wrap_gap(gap, lengths[component])
        offset = frac_tiles[component][target][:, :, None] - frac_tiles[component][source][:, None, :]
        deltas.append(gap.astype(jnp.float32) + offset)
    distance = deltas[0] * deltas[0] + deltas[1] * deltas[1] + deltas[2] * deltas[2]
    softened = distance + EPS_SQ
    falloff = NEAR_SCALE * jnp.exp(-distance / RANGE_SQ) / (softened * jnp.sqrt(softened))
    diagonal = (distance + 2.0 * EPS_SQ) * falloff
    pulled = [force_tiles[component][source][:, None, :] for component in range(3)]
    along = deltas[0] * pulled[0] + deltas[1] * pulled[1] + deltas[2] * pulled[2]
    live = (jnp.arange(slots, dtype=jnp.int32) < count).astype(jnp.float32)[:, None]
    return jnp.stack([lax.optimization_barrier(jnp.sum(diagonal * pulled[component] + falloff * deltas[component] * along, axis=2)) * live for component in range(3)])

def near_block(items):
    stencil_start, fraction, forces, pairs, count = items
    tiles = stencil_start.shape[1] // 128
    terms = pair_terms(stencil_start, fraction, forces, pairs, count)
    near = jnp.zeros((3, tiles, 128), jnp.float32).at[:, pairs[:, 0]].add(terms)
    return near.reshape(3, tiles * 128)

def reference(forces, stencil_start, fraction, tile_pairs, pair_count):
    weights = spline_weights(fraction)
    grid = jnp.zeros((3, NX, NY, NZ), jnp.float32)
    cells = []
    for step_x in range(4):
        for step_y in range(4):
            for step_z in range(4):
                index_x = (stencil_start[0] + step_x) % NX
                index_y = (stencil_start[1] + step_y) % NY
                index_z = (stencil_start[2] + step_z) % NZ
                weight = weights[step_x][0] * weights[step_y][1] * weights[step_z][2]
                cells.append((index_x, index_y, index_z, weight))
                grid = grid.at[:, index_x, index_y, index_z].add(forces * weight)
    spectrum = jnp.fft.fftn(grid, axes=(1, 2, 3))
    wave_x, keep_x = wave_numbers(jnp.arange(NX, dtype=jnp.int32), NX)
    wave_y, keep_y = wave_numbers(jnp.arange(NY, dtype=jnp.int32), NY)
    wave_z, keep_z = wave_numbers(jnp.arange(NZ, dtype=jnp.int32), NZ)
    wave_x = wave_x[:, None, None]
    wave_y = wave_y[None, :, None]
    wave_z = wave_z[None, None, :]
    squared = wave_x * wave_x + wave_y * wave_y + wave_z * wave_z
    anchor = squared == 0
    keep = keep_x[:, None, None] & keep_y[None, :, None] & keep_z[None, None, :] & jnp.logical_not(anchor)
    inverse = jnp.where(keep, 1.0 / jnp.where(anchor, 1.0, squared), 0.0)
    project = (wave_x * spectrum[0] + wave_y * spectrum[1] + wave_z * spectrum[2]) * inverse
    flow = jnp.stack([(spectrum[0] - wave_x * project) * inverse, (spectrum[1] - wave_y * project) * inverse, (spectrum[2] - wave_z * project) * inverse])
    field = jnp.real(jnp.fft.ifftn(flow, axes=(1, 2, 3))).astype(jnp.float32)
    far = jnp.zeros_like(forces)
    for index_x, index_y, index_z, weight in cells:
        far = far + field[:, index_x, index_y, index_z] * weight
    blocks = NPTS // PD
    near = lax.map(near_block, (stencil_start.reshape(3, blocks, PD).transpose(1, 0, 2), fraction.reshape(3, blocks, PD).transpose(1, 0, 2), forces.reshape(3, blocks, PD).transpose(1, 0, 2), tile_pairs.reshape(blocks, TL, 2), pair_count))
    near = near.transpose(1, 0, 2).reshape(3, NPTS)
    return far + near
```

```python
import functools

import jax
import jax.numpy as jnp
import numpy as np
from jax import lax
from jax.experimental import pallas as pl
from jax.experimental.pallas import tpu as pltpu
from jax.sharding import PartitionSpec as P

NX = 1024
NY = 128
NZ = 128
MESH = pl.DeviceIdType.MESH
F32 = jnp.float32
BF16 = jnp.bfloat16
TWO_PI = 2.0 * np.pi
CHUNK = 256
VMEM = pltpu.VMEM
SLOTS = 48


def halves(table):
    table = np.asarray(table, np.float32)
    high = table.astype(BF16)
    low = (table - high.astype(np.float32)).astype(BF16)
    return jnp.asarray(high), jnp.asarray(low)


def make_tables():
    k = np.arange(64)[:, None]
    z = np.arange(128)[None, :]
    angle = TWO_PI * ((k * z) % 128) / 128
    forward_z = np.concatenate([np.cos(angle), -np.sin(angle)], 0)
    weight = np.where(k == 0, 1.0, 2.0) / float(NX * NY * NZ)
    back_z = np.concatenate([weight * np.cos(angle), -weight * np.sin(angle)], 0)
    n = np.arange(128)
    angle = TWO_PI * ((n[:, None] * n[None, :]) % 128) / 128
    table_y = np.concatenate([np.cos(angle), np.sin(angle)], 1)
    n = np.arange(256)
    angle = TWO_PI * ((n[:, None] * n[None, :]) % 256) / 256
    cosine, sine = np.cos(angle), np.sin(angle)
    forward_x = np.zeros((2, 256, 256, 2))
    forward_x[0, :, :, 0] = cosine
    forward_x[0, :, :, 1] = sine
    forward_x[1, :, :, 0] = -sine
    forward_x[1, :, :, 1] = cosine
    forward_x = forward_x.reshape(512, 512)
    mix = np.zeros((2, 4, 32, 2, 4, 32))
    for r in range(4):
        for x in range(4):
            factor = (-1j) ** (r * x)
            for lane in range(32):
                mix[0, x, lane, 0, r, lane] = round(factor.real)
                mix[0, x, lane, 1, r, lane] = round(factor.imag)
                mix[1, x, lane, 0, r, lane] = -round(factor.imag)
                mix[1, x, lane, 1, r, lane] = round(factor.real)
    mix = mix.reshape(256, 256)
    q = np.arange(256)[:, None]
    x = (np.arange(128) // 32)[None, :]
    angle = TWO_PI * ((q * x) % 1024) / 1024
    return dict(
        forward_z=halves(forward_z),
        back_z=halves(back_z),
        table_y=halves(table_y),
        forward_x=halves(forward_x),
        back_x=halves(forward_x.T),
        mix=jnp.asarray(mix.astype(BF16)),
        unmix=jnp.asarray(mix.T.astype(BF16)),
        turn=(jnp.asarray(np.cos(angle).astype(np.float32)), jnp.asarray(np.sin(angle).astype(np.float32))),
    )


def split(value):
    high = value.astype(BF16)
    low = (value - high.astype(F32)).astype(BF16)
    return high, low


def mm(a, b):
    return jnp.dot(a, b, preferred_element_type=F32)


def mm3(a, b):
    return mm(a[0], b[0]) + (mm(a[0], b[1]) + mm(a[1], b[0]))


def spline_weights(t):
    square = t * t
    cube = square * t
    rest = 1.0 - t
    return [
        rest * rest * rest / 6.0,
        (3.0 * cube - 6.0 * square + 4.0) / 6.0,
        (-3.0 * cube + 3.0 * square + 3.0 * t + 1.0) / 6.0,
        cube / 6.0,
    ]


def line_weights(start, weights, dim):
    rows = lax.broadcasted_iota(jnp.int32, (128, start.shape[1]), 0)
    at = (rows - start[dim : dim + 1]) & 127
    result = jnp.zeros(at.shape, F32)
    for j in range(4):
        result = jnp.where(at == j, weights[j][dim : dim + 1], result)
    return result


def plane_weights(start, weights, planes):
    offset = start[0:1] & 3
    result = []
    for plane in planes:
        total = jnp.zeros(offset.shape, F32)
        for j in range(4):
            total = jnp.where(offset + j == plane, weights[j][0:1], total)
        result.append(total)
    return result


def swap_blocks(a):
    lane = lax.broadcasted_iota(jnp.int32, a[0].shape, 1)
    wide = lane < 64
    narrow = (lane & 63) < 32
    b = [None] * 4
    for i in range(2):
        b[i] = jnp.where(wide, a[i], pltpu.roll(a[i + 2], 64, 1))
        b[i + 2] = jnp.where(wide, pltpu.roll(a[i], 64, 1), a[i + 2])
    o = [None] * 4
    for i in (0, 2):
        o[i] = jnp.where(narrow, b[i], pltpu.roll(b[i + 1], 32, 1))
        o[i + 1] = jnp.where(narrow, pltpu.roll(b[i], 96, 1), b[i + 1])
    return o


def spread_step(planes, stride, start_ref, fraction_ref, force_ref, table, acc, left_high, left_low):
    start = start_ref[...]
    weights = spline_weights(fraction_ref[...])
    force = force_ref[...]
    y = split(line_weights(start, weights, 1))
    right = jnp.concatenate(y, axis=0)
    z = mm3(table, split(line_weights(start, weights, 2)))
    along = plane_weights(start, weights, planes)
    count = len(planes)
    for c in range(3):
        for i in range(count):
            high, low = split(z * (force[c : c + 1] * along[i]))
            left_high[pl.ds((c * count + i) * 128, 128), :] = high
            left_low[pl.ds((c * count + i) * 128, 128), :] = low
    for c in range(3):
        rows = pl.ds(c * count * 128, count * 128)
        dims = (((1,), (1,)), ((), ()))
        acc[pl.ds(c * stride * 128, count * 128), :] += lax.dot_general(
            left_high[rows, :], right, dims, preferred_element_type=F32
        ) + lax.dot_general(left_low[rows, :], right, dims, preferred_element_type=F32)


def spread_own_kernel(start, fraction, force, fz_high, fz_low, out, acc, left_high, left_low):
    step = pl.program_id(0)

    @pl.when(step == 0)
    def _():
        acc[...] = jnp.zeros_like(acc)

    spread_step(range(4), 4, start, fraction, force, (fz_high[...], fz_low[...]), acc, left_high, left_low)

    @pl.when(step == pl.num_programs(0) - 1)
    def _():
        out[...] = acc[:, :128] + acc[:, 128:]


def spread_behind_kernel(
    start, fraction, force, fz_high, fz_low, own, ty_high, ty_low, out, acc, left_high, left_low
):
    step = pl.program_id(0)

    @pl.when(step == 0)
    def _():
        acc[:, :128] = own[...]
        acc[:, 128:] = jnp.zeros_like(own)

    spread_step(range(4, 7), 4, start, fraction, force, (fz_high[...], fz_low[...]), acc, left_high, left_low)

    @pl.when(step == pl.num_programs(0) - 1)
    def _():
        for c in range(3):
            parts = []
            for x in range(4):
                rows = pl.ds((c * 4 + x) * 128, 128)
                value = split(acc[rows, :128] + acc[rows, 128:])
                value = mm3(value, (ty_high[...], ty_low[...]))
                re, im = value[:64], value[64:]
                parts.append((re[:, :128] + im[:, 128:], im[:, :128] - re[:, 128:]))
            for part in range(2):
                blocks = swap_blocks([p[part] for p in parts])
                for q in range(4):
                    out[c, pl.ds(q * 128 + part, 64, stride=2), :] = blocks[q]


def point_spec():
    return pl.BlockSpec((3, CHUNK), lambda i: (0, i))


def whole(shape):
    return pl.BlockSpec(shape, lambda i: (0,) * len(shape))


def cost(flops):
    return pl.CostEstimate(flops=flops, bytes_accessed=4000000, transcendentals=0)


def spread_own(points, tables):
    steps = points[0].shape[1] // CHUNK
    return pl.pallas_call(
        spread_own_kernel,
        grid=(steps,),
        in_specs=[point_spec()] * 3 + [whole((128, 128))] * 2,
        out_specs=whole((1536, 128)),
        out_shape=jax.ShapeDtypeStruct((1536, 128), F32),
        scratch_shapes=[VMEM((1536, 256), F32), VMEM((1536, CHUNK), BF16), VMEM((1536, CHUNK), BF16)],
        cost_estimate=cost(4000000000),
        name="spread_own",
    )(*points, *tables["forward_z"])


def spread_behind(points, own, tables):
    steps = points[0].shape[1] // CHUNK
    return pl.pallas_call(
        spread_behind_kernel,
        grid=(steps,),
        in_specs=[point_spec()] * 3
        + [whole((128, 128))] * 2
        + [whole((1536, 128))]
        + [whole((128, 256))] * 2,
        out_specs=whole((3, 512, 128)),
        out_shape=jax.ShapeDtypeStruct((3, 512, 128), F32),
        scratch_shapes=[VMEM((1536, 256), F32), VMEM((1152, CHUNK), BF16), VMEM((1152, CHUNK), BF16)],
        cost_estimate=cost(4000000000),
        name="spread_behind",
    )(*points, *tables["forward_z"], own, *tables["table_y"])


def near_terms(tiles, terms):
    def slot(s, carry):
        row = tiles[s]
        col = tiles[SLOTS + s].T
        gap = []
        for d in range(3):
            whole_gap = row[d : d + 1] - col[:, d : d + 1]
            if d > 0:
                whole_gap = jnp.where(whole_gap > 64.0, whole_gap - 128.0, whole_gap)
                whole_gap = jnp.where(whole_gap < -64.0, whole_gap + 128.0, whole_gap)
            gap.append(whole_gap + (row[3 + d : 4 + d] - col[:, 3 + d : 4 + d]))
        distance = gap[0] * gap[0] + gap[1] * gap[1] + gap[2] * gap[2]
        inverse = lax.rsqrt(distance + 1.0)
        fall = 0.25 * jnp.exp(distance * (-1.0 / 16.0)) * (inverse * inverse * inverse)
        pulled = [col[:, 6 + c : 7 + c] for c in range(3)]
        along = (gap[0] * pulled[0] + gap[1] * pulled[1] + gap[2] * pulled[2]) * fall
        diagonal = (distance + 2.0) * fall
        for c in range(3):
            term = diagonal * pulled[c] + along * gap[c]
            terms[c, pl.ds(s, 1), :] = jnp.sum(term, axis=0, keepdims=True)
        return carry

    lax.fori_loop(0, SLOTS, slot, 0)


def exchange_kernel(
    send, fx_high, fx_low, bx_high, bx_low, mix, unmix, turn_cos, turn_sin, tiles,
    out, terms, mid_a, held, back, mid_b, modes, send_sem, recv_sem, local_sem,
):
    me = lax.axis_index("group") * 128 + lax.axis_index("dev")
    yx = me >> 4
    zc = me & 15

    def at(yx_, zc_):
        index = yx_ * 16 + zc_
        return (index >> 7, index & 127)

    barrier = pltpu.get_barrier_semaphore()
    for j in range(1, 16):
        pl.semaphore_signal(barrier, inc=1, device_id=at(yx, (zc + j) & 15), device_id_type=MESH)
        pl.semaphore_signal(barrier, inc=1, device_id=at((yx + j) & 15, zc), device_id_type=MESH)
    pl.semaphore_wait(barrier, 30)

    def phase(number, c, source, target, along_z):
        here = zc if along_z else yx
        pltpu.make_async_copy(source(here), target, local_sem.at[number, c]).start()
        for j in range(1, 16):
            there = (here + j) & 15
            pltpu.make_async_remote_copy(
                src_ref=source(there),
                dst_ref=target,
                send_sem=send_sem.at[number, c],
                recv_sem=recv_sem.at[number, c],
                device_id=at(yx, there) if along_z else at(there, zc),
                device_id_type=MESH,
            ).start()

    def finish(number, c, source, target, whole_source, whole_target):
        pltpu.make_async_copy(source, target, local_sem.at[number, c]).wait()
        everything = pltpu.make_async_remote_copy(
            src_ref=whole_source,
            dst_ref=whole_target,
            send_sem=send_sem.at[number, c],
            recv_sem=recv_sem.at[number, c],
            device_id=at(yx, zc),
            device_id_type=MESH,
        )
        everything.wait_recv()
        everything.wait_send()

    most = pl.ds(0, 15)
    for c in range(3):
        phase(0, c, lambda z, c=c: send.at[c, z], mid_a.at[c, zc], True)
    near_terms(tiles, terms)
    for c in range(3):
        finish(0, c, send.at[c, zc], mid_a.at[c, zc], send.at[c, most], mid_a.at[c, most])
        phase(1, c, lambda y, c=c: mid_a.at[c, :, y], held.at[c, yx], False)

    cos, sin = turn_cos[...], turn_sin[...]
    for c in range(3):
        finish(1, c, mid_a.at[c, :, yx], held.at[c, yx], held.at[c, most], held.at[c, most])
        value = split(held.reshape(3, 512, 128)[c])
        both = jnp.concatenate(value, axis=1)
        top = mm(fx_high[...], both)
        value = top[:, :128] + (top[:, 128:] + mm(fx_low[...], value[0]))
        re, im = value[:256], value[256:]
        turned = jnp.concatenate([re * cos + im * sin, im * cos - re * sin], axis=1)
        high, low = split(turned)
        modes[c] = mm(high, mix[...]) + mm(low, mix[...])

    column = zc * 16 + yx
    lane = lax.broadcasted_iota(jnp.int32, (256, 128), 1)
    row = lax.broadcasted_iota(jnp.int32, (256, 128), 0)
    index_x = row + 256 * (lane >> 5)
    index_y = (lane & 31) + 32 * (column >> 6)
    index_z = column & 63
    step_x = TWO_PI / NX
    step_y = TWO_PI / NY
    wave_x = jnp.where(index_x > 512, index_x - 1024, index_x).astype(F32) * step_x
    wave_y = jnp.where(index_y > 64, index_y - 128, index_y).astype(F32) * step_y
    wave_z = index_z.astype(F32) * step_y
    squared = wave_x * wave_x + wave_y * wave_y + wave_z * wave_z
    anchor = squared == 0.0
    drop = anchor | (index_x == 512) | (index_y == 64)
    inverse = jnp.where(drop, 0.0, 1.0 / jnp.where(anchor, 1.0, squared))
    waves = (wave_x, wave_y, wave_z)
    for part in range(2):
        lanes = slice(part * 128, part * 128 + 128)
        values = [modes[c, :, lanes] for c in range(3)]
        project = (wave_x * values[0] + wave_y * values[1] + wave_z * values[2]) * inverse
        for c in range(3):
            modes[c, :, lanes] = (values[c] - waves[c] * project) * inverse

    for c in range(3):
        high, low = split(modes[c])
        value = mm(high, unmix[...]) + mm(low, unmix[...])
        re, im = value[:, :128], value[:, 128:]
        value = split(jnp.concatenate([re * cos - im * sin, im * cos + re * sin], axis=0))
        both = jnp.concatenate(value, axis=1)
        top = mm(bx_high[...], both)
        back.reshape(3, 512, 128)[c] = top[:, :128] + (top[:, 128:] + mm(bx_low[...], value[0]))
        phase(2, c, lambda y, c=c: back.at[c, y], mid_b.at[c, yx], False)
    for c in range(3):
        finish(2, c, back.at[c, yx], mid_b.at[c, yx], back.at[c, most], mid_b.at[c, most])
        phase(3, c, lambda z, c=c: mid_b.at[c, :, z], out.at[c, zc], True)
    for c in range(3):
        finish(3, c, mid_b.at[c, :, zc], out.at[c, zc], out.at[c, most], out.at[c, most])


def exchange(send, tiles, tables):
    shape = (3, 16, 16, 2, 128)
    vmem = pl.BlockSpec(memory_space=pltpu.VMEM)
    return pl.pallas_call(
        exchange_kernel,
        in_specs=[vmem] * 10,
        out_specs=[vmem, vmem],
        out_shape=[jax.ShapeDtypeStruct(shape, F32), jax.ShapeDtypeStruct((3, SLOTS, 128), F32)],
        scratch_shapes=[VMEM(shape, F32)] * 4
        + [VMEM((3, 256, 256), F32)]
        + [pltpu.SemaphoreType.DMA((4, 3))] * 3,
        compiler_params=pltpu.CompilerParams(collective_id=0, has_side_effects=True),
        name="exchange",
    )(
        send.reshape(shape),
        *tables["forward_x"],
        *tables["back_x"],
        tables["mix"],
        tables["unmix"],
        *tables["turn"],
        tiles,
    )


def gather_step(planes, start_ref, fraction_ref, table, left, out):
    start = start_ref[...]
    weights = spline_weights(fraction_ref[...])
    y_high, y_low = split(line_weights(start, weights, 1))
    z = mm3(table, split(line_weights(start, weights, 2)))
    along = plane_weights(start, weights, planes)
    twice = jnp.concatenate([y_high, y_high], axis=0)
    for c in range(3):
        total = jnp.zeros_like(z)
        for i in range(len(planes)):
            rows = pl.ds((c * 4 + i) * 128, 128)
            both = left[rows, :]
            value = mm(both, twice) + mm(both[:, :128], y_low)
            total = total + value * along[i]
        out[c : c + 1, :] = jnp.sum(total * z, axis=0, keepdims=True)


def gather_behind_kernel(start, fraction, bz_high, bz_low, ty_high, ty_low, lines, out, left):
    @pl.when(pl.program_id(0) == 0)
    def _():
        for c in range(3):
            parts = []
            for part in range(2):
                parts.append(
                    swap_blocks([lines[c, pl.ds(q * 128 + part, 64, stride=2), :] for q in range(4)])
                )
            for x in range(4):
                value = split(jnp.concatenate([parts[0][x], parts[1][x]], axis=0))
                value = mm3(value, (ty_high[...], ty_low[...]))
                re, im = value[:64], value[64:]
                plane = jnp.concatenate([re[:, :128] - im[:, 128:], im[:, :128] + re[:, 128:]], axis=0)
                left[pl.ds((c * 4 + x) * 128, 128), :] = jnp.concatenate(split(plane), axis=1)

    gather_step(range(4, 7), start, fraction, (bz_high[...], bz_low[...]), left, out)


def gather_own_kernel(start, fraction, bz_high, bz_low, left, out):
    gather_step(range(4), start, fraction, (bz_high[...], bz_low[...]), left, out)


def gather_behind(points, lines, tables):
    count = points[0].shape[1]
    return pl.pallas_call(
        gather_behind_kernel,
        grid=(count // CHUNK,),
        in_specs=[point_spec()] * 2
        + [whole((128, 128))] * 2
        + [whole((128, 256))] * 2
        + [whole((3, 512, 128))],
        out_specs=[point_spec(), whole((1536, 256))],
        out_shape=[jax.ShapeDtypeStruct((3, count), F32), jax.ShapeDtypeStruct((1536, 256), BF16)],
        cost_estimate=cost(4000000000),
        name="gather_behind",
    )(*points[:2], *tables["back_z"], *tables["table_y"], lines)


def gather_own(points, left, tables):
    count = points[0].shape[1]
    return pl.pallas_call(
        gather_own_kernel,
        grid=(count // CHUNK,),
        in_specs=[point_spec()] * 2 + [whole((128, 128))] * 2 + [whole((1536, 256))],
        out_specs=point_spec(),
        out_shape=jax.ShapeDtypeStruct((3, count), F32),
        cost_estimate=cost(4000000000),
        name="gather_own",
    )(*points[:2], *tables["back_z"], left)


def from_behind(x, by):
    return lax.ppermute(x, ("group", "dev"), [(i, (i + by) % 256) for i in range(256)])


def per_device(tables, forces, stencil_start, fraction, tile_pairs, pair_count):
    count = forces.shape[1]
    tiles = count // 128
    own = (stencil_start, fraction, forces)
    start_float = stencil_start.astype(F32)
    packed = jnp.concatenate([start_float, fraction, forces], axis=0)
    behind = from_behind(packed, 1)
    behind = (behind[0:3].astype(jnp.int32), behind[3:6], behind[6:9])
    slab = spread_own(own, tables)
    send = spread_behind(behind, slab, tables)
    spots = jnp.arange(tiles, dtype=jnp.int32)[None, :]
    padded = jnp.concatenate([packed, jnp.zeros((7, count), F32)], axis=0)
    ends = (jnp.concatenate([tile_pairs[:, 0], tile_pairs[:, 1]])[:, None] == spots).astype(F32)
    picked = jnp.einsum(
        "st,ktp->skp", ends, padded.reshape(16, tiles, 128), precision=lax.Precision.HIGHEST
    )
    lines, terms = exchange(send, picked, tables)
    partial, left = gather_behind(behind, lines.reshape(3, 512, 128), tables)
    partial = from_behind(partial, -1)
    far = gather_own(own, left, tables)
    live = jnp.arange(SLOTS, dtype=jnp.int32) < pair_count[0]
    onehot = jnp.where(live[:, None], ends[:SLOTS], 0.0)
    near = jnp.einsum("st,csp->ctp", onehot, terms, precision=lax.Precision.HIGHEST)
    return far + near.reshape(3, count) + partial


def solution(mesh):
    tables = make_tables()
    in_specs = (
        P(None, ("group", "dev")),
        P(None, ("group", "dev")),
        P(None, ("group", "dev")),
        P(("group", "dev"), None),
        P(("group", "dev")),
    )
    return jax.shard_map(
        functools.partial(per_device, tables),
        mesh=mesh,
        in_specs=in_specs,
        out_specs=P(None, ("group", "dev")),
        check_vma=False,
    )
```

```python
import functools

import jax
import jax.numpy as jnp
import numpy as np
from jax import lax
from jax.experimental import pallas as pl
from jax.experimental.pallas import tpu as pltpu
from jax.sharding import PartitionSpec as P

NX = 1024
NY = 128
NZ = 128
MESH = pl.DeviceIdType.MESH
F32 = jnp.float32
BF16 = jnp.bfloat16
TWO_PI = 2.0 * np.pi
CHUNK = 512
VMEM = pltpu.VMEM
SLOTS = 48


def halves(table):
    table = np.asarray(table, np.float32)
    high = table.astype(BF16)
    low = (table - high.astype(np.float32)).astype(BF16)
    return jnp.asarray(high), jnp.asarray(low)


def make_tables():
    k = np.arange(64)[:, None]
    z = np.arange(128)[None, :]
    angle = TWO_PI * ((k * z) % 128) / 128
    forward_z = np.concatenate([np.cos(angle), -np.sin(angle)], 0)
    weight = np.where(k == 0, 1.0, 2.0) / float(NX * NY * NZ)
    back_z = np.concatenate([weight * np.cos(angle), -weight * np.sin(angle)], 0)
    n = np.arange(128)
    angle = TWO_PI * ((n[:, None] * n[None, :]) % 128) / 128
    table_y = np.concatenate([np.cos(angle), np.sin(angle)], 1)
    n = np.arange(256)
    angle = TWO_PI * ((n[:, None] * n[None, :]) % 256) / 256
    cosine, sine = np.cos(angle), np.sin(angle)
    forward_x = np.zeros((2, 256, 256, 2))
    forward_x[0, :, :, 0] = cosine
    forward_x[0, :, :, 1] = sine
    forward_x[1, :, :, 0] = -sine
    forward_x[1, :, :, 1] = cosine
    forward_x = forward_x.reshape(512, 512)
    mix = np.zeros((2, 4, 32, 2, 4, 32))
    for r in range(4):
        for x in range(4):
            factor = (-1j) ** (r * x)
            for lane in range(32):
                mix[0, x, lane, 0, r, lane] = round(factor.real)
                mix[0, x, lane, 1, r, lane] = round(factor.imag)
                mix[1, x, lane, 0, r, lane] = -round(factor.imag)
                mix[1, x, lane, 1, r, lane] = round(factor.real)
    mix = mix.reshape(256, 256)
    q = np.arange(256)[:, None]
    x = (np.arange(128) // 32)[None, :]
    angle = TWO_PI * ((q * x) % 1024) / 1024
    return dict(
        forward_z=halves(forward_z),
        back_z=halves(back_z),
        table_y=halves(table_y),
        forward_x=halves(forward_x),
        back_x=halves(forward_x.T),
        mix=jnp.asarray(mix.astype(BF16)),
        unmix=jnp.asarray(mix.T.astype(BF16)),
        turn=(jnp.asarray(np.cos(angle).astype(np.float32)), jnp.asarray(np.sin(angle).astype(np.float32))),
    )


def split(value):
    high = value.astype(BF16)
    low = (value - high.astype(F32)).astype(BF16)
    return high, low


def mm(a, b):
    return jnp.dot(a, b, preferred_element_type=F32)


def mm3(a, b):
    return mm(a[0], b[0]) + (mm(a[0], b[1]) + mm(a[1], b[0]))


def spline_weights(t):
    square = t * t
    cube = square * t
    rest = 1.0 - t
    return [
        rest * rest * rest / 6.0,
        (3.0 * cube - 6.0 * square + 4.0) / 6.0,
        (-3.0 * cube + 3.0 * square + 3.0 * t + 1.0) / 6.0,
        cube / 6.0,
    ]


def line_weights(start, weights, dim):
    rows = lax.broadcasted_iota(jnp.int32, (128, start.shape[1]), 0)
    at = (rows - start[dim : dim + 1]) & 127
    result = jnp.zeros(at.shape, F32)
    for j in range(4):
        result = jnp.where(at == j, weights[j][dim : dim + 1], result)
    return result


def plane_weights(start, weights, planes):
    offset = start[0:1] & 3
    result = []
    for plane in planes:
        total = jnp.zeros(offset.shape, F32)
        for j in range(4):
            total = jnp.where(offset + j == plane, weights[j][0:1], total)
        result.append(total)
    return result


def swap_blocks(a):
    lane = lax.broadcasted_iota(jnp.int32, a[0].shape, 1)
    wide = lane < 64
    narrow = (lane & 63) < 32
    b = [None] * 4
    for i in range(2):
        b[i] = jnp.where(wide, a[i], pltpu.roll(a[i + 2], 64, 1))
        b[i + 2] = jnp.where(wide, pltpu.roll(a[i], 64, 1), a[i + 2])
    o = [None] * 4
    for i in (0, 2):
        o[i] = jnp.where(narrow, b[i], pltpu.roll(b[i + 1], 32, 1))
        o[i + 1] = jnp.where(narrow, pltpu.roll(b[i], 96, 1), b[i + 1])
    return o


def prepare(start_ref, fraction_ref, table, y_pair, z_modes, along, planes):
    def step(k, carry):
        cols = pl.ds(pl.multiple_of(k * 256, 256), 256)
        start = start_ref[:, cols]
        weights = spline_weights(fraction_ref[:, cols])
        y_high, y_low = split(line_weights(start, weights, 1))
        y_pair[:128, cols] = y_high
        y_pair[128:, cols] = y_low
        z_modes[:, cols] = mm3(table, split(line_weights(start, weights, 2)))
        for i, row in enumerate(plane_weights(start, weights, planes)):
            along[i : i + 1, cols] = row
        return carry

    lax.fori_loop(0, start_ref.shape[1] // 256, step, 0)


def back_modes(start_ref, fraction_ref, table, z_modes):
    def step(k, carry):
        cols = pl.ds(pl.multiple_of(k * 256, 256), 256)
        weights = spline_weights(fraction_ref[:, cols])
        z_modes[:, cols] = mm3(table, split(line_weights(start_ref[:, cols], weights, 2)))
        return carry

    lax.fori_loop(0, start_ref.shape[1] // 256, step, 0)


def spread(c, count, force_ref, y_pair, z_modes, along, acc):
    def step(k, carry):
        cols = pl.ds(pl.multiple_of(k * CHUNK, CHUNK), CHUNK)
        z = z_modes[:, cols]
        right = y_pair[:, cols]
        force = force_ref[c : c + 1, cols]
        pieces = [split(z * (force * along[i : i + 1, cols])) for i in range(count)]
        high = jnp.concatenate([p[0] for p in pieces], axis=0)
        low = jnp.concatenate([p[1] for p in pieces], axis=0)
        dims = (((1,), (1,)), ((), ()))
        acc[c, : count * 128, :] += lax.dot_general(
            high, right, dims, preferred_element_type=F32
        ) + lax.dot_general(low, right, dims, preferred_element_type=F32)
        return carry

    lax.fori_loop(0, force_ref.shape[1] // CHUNK, step, 0)


def gather(c, count, y_pair, z_modes, along, left, out):
    def step(k, carry):
        cols = pl.ds(pl.multiple_of(k * CHUNK, CHUNK), CHUNK)
        pair = y_pair[:, cols]
        twice = jnp.concatenate([pair[:128], pair[:128]], axis=0)
        both = left[c, : count * 128, :]
        value = mm(both, twice) + mm(both[:, :128], pair[128:])
        total = value[:128] * along[0:1, cols]
        for i in range(1, count):
            total = total + value[i * 128 : i * 128 + 128] * along[i : i + 1, cols]
        out[c : c + 1, cols] = jnp.sum(total * z_modes[:, cols], axis=0, keepdims=True)
        return carry

    lax.fori_loop(0, out.shape[1] // CHUNK, step, 0)


def lines_forward(acc, c, table, send):
    parts = []
    for x in range(4):
        rows = pl.ds(x * 128, 128)
        value = mm3(split(acc[c, rows, :128] + acc[c, rows, 128:]), table)
        re, im = value[:64], value[64:]
        parts.append((re[:, :128] + im[:, 128:], im[:, :128] - re[:, 128:]))
    for part in range(2):
        blocks = swap_blocks([p[part] for p in parts])
        for q in range(4):
            send[c, pl.ds(q * 128 + part, 64, stride=2), :] = blocks[q]


def lines_back(lines, c, table, left):
    parts = []
    for part in range(2):
        parts.append(swap_blocks([lines[c, pl.ds(q * 128 + part, 64, stride=2), :] for q in range(4)]))
    for x in range(4):
        value = mm3(split(jnp.concatenate([parts[0][x], parts[1][x]], axis=0)), table)
        re, im = value[:64], value[64:]
        plane = jnp.concatenate([re[:, :128] - im[:, 128:], im[:, :128] + re[:, 128:]], axis=0)
        left[c, pl.ds(x * 128, 128), :] = jnp.concatenate(split(plane), axis=1)


def pick_tiles(ends, start_ref, fraction_ref, force_ref, by_tile, tiles):
    count = start_ref.shape[1] // 128
    flat = by_tile.reshape(count * 16, 128)
    for t in range(count):
        cols = slice(t * 128, t * 128 + 128)
        by_tile[t, 0:3, :] = start_ref[:, cols].astype(F32)
        by_tile[t, 3:6, :] = fraction_ref[:, cols]
        by_tile[t, 6:9, :] = force_ref[:, cols]
    target = tiles.reshape(2 * SLOTS * 16, 128)
    for k in range(9):
        target[pl.ds(k, 2 * SLOTS, stride=16), :] = jnp.dot(
            ends[...],
            flat[pl.ds(k, count, stride=16), :],
            precision=lax.Precision.HIGHEST,
            preferred_element_type=F32,
        )


def near_sum(live, terms, near):
    for c in range(3):
        value = lax.dot_general(
            live[...],
            terms[c],
            (((0,), (0,)), ((), ())),
            precision=lax.Precision.HIGHEST,
            preferred_element_type=F32,
        )
        for t in range(value.shape[0]):
            near[c : c + 1, t * 128 : t * 128 + 128] = value[t : t + 1]


def near_terms(tiles, terms):
    def slot(s, carry):
        row = tiles[s]
        col = tiles[SLOTS + s].T
        gap = []
        for d in range(3):
            whole_gap = row[d : d + 1] - col[:, d : d + 1]
            if d > 0:
                whole_gap = jnp.where(whole_gap > 64.0, whole_gap - 128.0, whole_gap)
                whole_gap = jnp.where(whole_gap < -64.0, whole_gap + 128.0, whole_gap)
            gap.append(whole_gap + (row[3 + d : 4 + d] - col[:, 3 + d : 4 + d]))
        distance = gap[0] * gap[0] + gap[1] * gap[1] + gap[2] * gap[2]
        inverse = lax.rsqrt(distance + 1.0)
        fall = 0.25 * jnp.exp(distance * (-1.0 / 16.0)) * (inverse * inverse * inverse)
        pulled = [col[:, 6 + c : 7 + c] for c in range(3)]
        along = (gap[0] * pulled[0] + gap[1] * pulled[1] + gap[2] * pulled[2]) * fall
        diagonal = (distance + 2.0) * fall
        for c in range(3):
            term = diagonal * pulled[c] + along * gap[c]
            terms[c, pl.ds(s, 1), :] = jnp.sum(term, axis=0, keepdims=True)
        return carry

    lax.fori_loop(0, SLOTS, slot, 0)


def step_kernel(
    start, fraction, force, ends, live, fz_high, fz_low, bz_high, bz_low, ty_high, ty_low,
    fx_high_far, fx_low_far, bx_high_far, bx_low_far, mix_far, unmix_far, cos_far, sin_far,
    out,
    start_b, fraction_b, force_b, y_pair, z_modes, along, acc, left, by_tile, tiles, terms, near,
    fx_high, fx_low, bx_high, bx_low, mix, unmix, turn_cos, turn_sin,
    send, mid_a, held, back, mid_b, lines, modes, partial, partial_in,
    send_sem, recv_sem, local_sem, table_sem, point_send, point_recv, last_send, last_recv,
):
    me = lax.axis_index("group") * 128 + lax.axis_index("dev")
    yx = me >> 4
    zc = me & 15

    def at(yx_, zc_):
        index = yx_ * 16 + zc_
        return (index >> 7, index & 127)

    def near_by(by):
        index = (me + by) & 255
        return (index >> 7, index & 127)

    barrier = pltpu.get_barrier_semaphore()
    for by in (1, 255):
        pl.semaphore_signal(barrier, inc=1, device_id=near_by(by), device_id_type=MESH)
    for j in range(1, 16):
        pl.semaphore_signal(barrier, inc=1, device_id=at(yx, (zc + j) & 15), device_id_type=MESH)
        pl.semaphore_signal(barrier, inc=1, device_id=at((yx + j) & 15, zc), device_id_type=MESH)

    table_copies = [
        pltpu.make_async_copy(source, target, table_sem.at[i])
        for i, (source, target) in enumerate(
            [
                (fx_high_far, fx_high), (fx_low_far, fx_low), (bx_high_far, bx_high), (bx_low_far, bx_low),
                (mix_far, mix), (unmix_far, unmix), (cos_far, turn_cos), (sin_far, turn_sin),
            ]
        )
    ]
    for copy in table_copies:
        copy.start()

    shape = (3, 16, 16, 2, 128)
    send_blocks, back_blocks, lines_blocks = send.reshape(shape), back.reshape(shape), lines.reshape(shape)
    most = pl.ds(0, 15)

    def phase(number, c, source, target, along_z):
        here = zc if along_z else yx
        pltpu.make_async_copy(source(here), target, local_sem.at[number, c]).start()
        for j in range(1, 16):
            there = (here + j) & 15
            pltpu.make_async_remote_copy(
                src_ref=source(there),
                dst_ref=target,
                send_sem=send_sem.at[number, c],
                recv_sem=recv_sem.at[number, c],
                device_id=at(yx, there) if along_z else at(there, zc),
                device_id_type=MESH,
            ).start()

    def finish(number, c, source, target, whole_source, whole_target):
        pltpu.make_async_copy(source, target, local_sem.at[number, c]).wait()
        everything = pltpu.make_async_remote_copy(
            src_ref=whole_source,
            dst_ref=whole_target,
            send_sem=send_sem.at[number, c],
            recv_sem=recv_sem.at[number, c],
            device_id=near_by(1),
            device_id_type=MESH,
        )
        everything.wait_recv()
        everything.wait_send()

    table_z = (fz_high[...], fz_low[...])
    table_y = (ty_high[...], ty_low[...])
    y_own, z_own, a_own = y_pair.at[0], z_modes.at[0], along.at[0]
    y_behind, z_behind, a_behind = y_pair.at[1], z_modes.at[1], along.at[1]

    acc[...] = jnp.zeros_like(acc)
    prepare(start, fraction, table_z, y_own, z_own, a_own, range(4))
    spread(0, 4, force, y_own, z_own, a_own, acc)
    pl.semaphore_wait(barrier, 32)
    points = [
        pltpu.make_async_remote_copy(
            src_ref=source,
            dst_ref=target,
            send_sem=point_send.at[i],
            recv_sem=point_recv.at[i],
            device_id=near_by(1),
            device_id_type=MESH,
        )
        for i, (source, target) in enumerate([(start, start_b), (fraction, fraction_b), (force, force_b)])
    ]
    for copy in points:
        copy.start()
    spread(1, 4, force, y_own, z_own, a_own, acc)
    for copy in points:
        copy.wait()
    prepare(start_b, fraction_b, table_z, y_behind, z_behind, a_behind, range(4, 7))
    for c in range(3):
        if c == 2:
            spread(2, 4, force, y_own, z_own, a_own, acc)
        spread(c, 3, force_b, y_behind, z_behind, a_behind, acc)
        lines_forward(acc, c, table_y, send)
        phase(0, c, lambda z, c=c: send_blocks.at[c, z], mid_a.at[c, zc], True)

    def half_way(c):
        finish(0, c, send_blocks.at[c, zc], mid_a.at[c, zc], send_blocks.at[c, most], mid_a.at[c, most])
        phase(1, c, lambda y, c=c: mid_a.at[c, :, y], held.at[c, yx], False)

    def line_modes(c):
        finish(1, c, mid_a.at[c, :, yx], held.at[c, yx], held.at[c, most], held.at[c, most])
        value = split(held.reshape(3, 512, 128)[c])
        both = jnp.concatenate(value, axis=1)
        top = mm(fx_high[...], both)
        value = top[:, :128] + (top[:, 128:] + mm(fx_low[...], value[0]))
        re, im = value[:256], value[256:]
        cos, sin = turn_cos[...], turn_sin[...]
        turned = jnp.concatenate([re * cos + im * sin, im * cos - re * sin], axis=1)
        high, low = split(turned)
        modes[c] = mm(high, mix[...]) + mm(low, mix[...])

    half_way(0)
    pick_tiles(ends, start, fraction, force, by_tile, tiles)
    near_terms(tiles, terms)
    for copy in table_copies:
        copy.wait()
    half_way(1)
    line_modes(0)
    near_sum(live, terms, near)
    back_modes(start, fraction, (bz_high[...], bz_low[...]), z_own)
    back_modes(start_b, fraction_b, (bz_high[...], bz_low[...]), z_behind)
    half_way(2)
    line_modes(1)
    line_modes(2)

    column = zc * 16 + yx
    lane = lax.broadcasted_iota(jnp.int32, (256, 128), 1)
    row = lax.broadcasted_iota(jnp.int32, (256, 128), 0)
    index_x = row + 256 * (lane >> 5)
    index_y = (lane & 31) + 32 * (column >> 6)
    index_z = column & 63
    step_x = TWO_PI / NX
    step_y = TWO_PI / NY
    wave_x = jnp.where(index_x > 512, index_x - 1024, index_x).astype(F32) * step_x
    wave_y = jnp.where(index_y > 64, index_y - 128, index_y).astype(F32) * step_y
    wave_z = index_z.astype(F32) * step_y
    squared = wave_x * wave_x + wave_y * wave_y + wave_z * wave_z
    anchor = squared == 0.0
    drop = anchor | (index_x == 512) | (index_y == 64)
    inverse = jnp.where(drop, 0.0, 1.0 / jnp.where(anchor, 1.0, squared))
    waves = (wave_x, wave_y, wave_z)
    for part in range(2):
        lanes = slice(part * 128, part * 128 + 128)
        values = [modes[c, :, lanes] for c in range(3)]
        project = (wave_x * values[0] + wave_y * values[1] + wave_z * values[2]) * inverse
        for c in range(3):
            modes[c, :, lanes] = (values[c] - waves[c] * project) * inverse

    for c in range(3):
        high, low = split(modes[c])
        value = mm(high, unmix[...]) + mm(low, unmix[...])
        re, im = value[:, :128], value[:, 128:]
        cos, sin = turn_cos[...], turn_sin[...]
        value = split(jnp.concatenate([re * cos - im * sin, im * cos + re * sin], axis=0))
        both = jnp.concatenate(value, axis=1)
        top = mm(bx_high[...], both)
        back[c] = top[:, :128] + (top[:, 128:] + mm(bx_low[...], value[0]))
        phase(2, c, lambda y, c=c: back_blocks.at[c, y], mid_b.at[c, yx], False)
    for c in range(3):
        finish(2, c, back_blocks.at[c, yx], mid_b.at[c, yx], back_blocks.at[c, most], mid_b.at[c, most])
        phase(3, c, lambda z, c=c: mid_b.at[c, :, z], lines_blocks.at[c, zc], True)

    last = pltpu.make_async_remote_copy(
        src_ref=partial,
        dst_ref=partial_in,
        send_sem=last_send,
        recv_sem=last_recv,
        device_id=near_by(255),
        device_id_type=MESH,
    )
    for c in range(3):
        finish(3, c, mid_b.at[c, :, zc], lines_blocks.at[c, zc], lines_blocks.at[c, most], lines_blocks.at[c, most])
        lines_back(lines, c, table_y, left)
        gather(c, 3, y_behind, z_behind, a_behind, left, partial)
        if c == 2:
            last.start()
        gather(c, 4, y_own, z_own, a_own, left, out)
    last.wait()
    out[...] = out[...] + near[...] + partial_in[...]


def step(forces, stencil_start, fraction, ends, live, tables):
    count = forces.shape[1]
    vmem = pl.BlockSpec(memory_space=pltpu.VMEM)
    far = pl.BlockSpec(memory_space=pl.ANY)
    blocks = (3, 16, 16, 2, 128)
    x_tables = [*tables["forward_x"], *tables["back_x"], tables["mix"], tables["unmix"], *tables["turn"]]
    dma = pltpu.SemaphoreType.DMA
    return pl.pallas_call(
        step_kernel,
        in_specs=[vmem] * 11 + [far] * 8,
        out_specs=vmem,
        out_shape=jax.ShapeDtypeStruct((3, count), F32),
        scratch_shapes=[
            VMEM((3, count), jnp.int32),
            VMEM((3, count), F32),
            VMEM((3, count), F32),
            VMEM((2, 256, count), BF16),
            VMEM((2, 128, count), F32),
            VMEM((2, 8, count), F32),
            VMEM((3, 512, 256), F32),
            VMEM((3, 512, 256), BF16),
            VMEM((count // 128, 16, 128), F32),
            VMEM((2 * SLOTS, 16, 128), F32),
            VMEM((3, SLOTS, 128), F32),
            VMEM((3, count), F32),
        ]
        + [VMEM(t.shape, t.dtype) for t in x_tables]
        + [
            VMEM((3, 512, 128), F32),
            VMEM(blocks, F32),
            VMEM(blocks, F32),
            VMEM((3, 512, 128), F32),
            VMEM(blocks, F32),
            VMEM((3, 512, 128), F32),
            VMEM((3, 256, 256), F32),
            VMEM((3, count), F32),
            VMEM((3, count), F32),
            dma((4, 3)),
            dma((4, 3)),
            dma((4, 3)),
            dma((8,)),
            dma((3,)),
            dma((3,)),
            dma,
            dma,
        ],
        compiler_params=pltpu.CompilerParams(collective_id=0, has_side_effects=True),
        name="step",
    )(
        stencil_start,
        fraction,
        forces,
        ends,
        live,
        *tables["forward_z"],
        *tables["back_z"],
        *tables["table_y"],
        *x_tables,
    )


def per_device(tables, forces, stencil_start, fraction, tile_pairs, pair_count):
    spots = jnp.arange(forces.shape[1] // 128, dtype=jnp.int32)[None, :]
    ends = (jnp.concatenate([tile_pairs[:, 0], tile_pairs[:, 1]])[:, None] == spots).astype(F32)
    used = jnp.arange(SLOTS, dtype=jnp.int32) < pair_count[0]
    live = jnp.where(used[:, None], ends[:SLOTS], 0.0)
    return step(forces, stencil_start, fraction, ends, live, tables)


def solution(mesh):
    tables = make_tables()
    in_specs = (
        P(None, ("group", "dev")),
        P(None, ("group", "dev")),
        P(None, ("group", "dev")),
        P(("group", "dev"), None),
        P(("group", "dev")),
    )
    return jax.shard_map(
        functools.partial(per_device, tables),
        mesh=mesh,
        in_specs=in_specs,
        out_specs=P(None, ("group", "dev")),
        check_vma=False,
    )
```

```python
import functools

import jax
import jax.numpy as jnp
import numpy as np
from jax import lax
from jax.experimental import pallas as pl
from jax.experimental.pallas import tpu as pltpu
from jax.sharding import PartitionSpec as P

NX = 1024
NY = 128
NZ = 128
MESH = pl.DeviceIdType.MESH
F32 = jnp.float32
BF16 = jnp.bfloat16
TWO_PI = 2.0 * np.pi
CHUNK = 512
VMEM = pltpu.VMEM
SLOTS = 48
LOG2_E = 1.4426950408889634


def halves(table):
    table = np.asarray(table, np.float32)
    high = table.astype(BF16)
    low = (table - high.astype(np.float32)).astype(BF16)
    return jnp.asarray(high), jnp.asarray(low)


def make_tables():
    k = np.arange(64)[:, None]
    z = np.arange(128)[None, :]
    angle = TWO_PI * ((k * z) % 128) / 128
    forward_z = np.concatenate([np.cos(angle), -np.sin(angle)], 0)
    weight = np.where(k == 0, 1.0, 2.0) / float(NX * NY * NZ)
    back_z = np.concatenate([weight * np.cos(angle), -weight * np.sin(angle)], 0)
    n = np.arange(128)
    angle = TWO_PI * ((n[:, None] * n[None, :]) % 128) / 128
    table_y = np.concatenate([np.cos(angle), np.sin(angle)], 1)
    n = np.arange(256)
    angle = TWO_PI * ((n[:, None] * n[None, :]) % 256) / 256
    cosine, sine = np.cos(angle), np.sin(angle)
    forward_x = np.zeros((2, 256, 256, 2))
    forward_x[0, :, :, 0] = cosine
    forward_x[0, :, :, 1] = sine
    forward_x[1, :, :, 0] = -sine
    forward_x[1, :, :, 1] = cosine
    forward_x = forward_x.reshape(512, 512)
    mix = np.zeros((2, 4, 32, 2, 4, 32))
    for r in range(4):
        for x in range(4):
            factor = (-1j) ** (r * x)
            for lane in range(32):
                mix[0, x, lane, 0, r, lane] = round(factor.real)
                mix[0, x, lane, 1, r, lane] = round(factor.imag)
                mix[1, x, lane, 0, r, lane] = -round(factor.imag)
                mix[1, x, lane, 1, r, lane] = round(factor.real)
    mix = mix.reshape(256, 256)
    q = np.arange(256)[:, None]
    x = (np.arange(128) // 32)[None, :]
    angle = TWO_PI * ((q * x) % 1024) / 1024
    return dict(
        forward_z=halves(forward_z),
        back_z=halves(back_z),
        table_y=halves(table_y),
        forward_x=halves(forward_x),
        mix=jnp.asarray(mix.astype(BF16)),
        unmix=jnp.asarray(mix.T.astype(BF16)),
        turn=(jnp.asarray(np.cos(angle).astype(np.float32)), jnp.asarray(np.sin(angle).astype(np.float32))),
    )


def split(value):
    high = value.astype(BF16)
    low = (value - high.astype(F32)).astype(BF16)
    return high, low


def mm(a, b):
    return jnp.dot(a, b, preferred_element_type=F32)


def mm3(a, b):
    return mm(a[0], b[0]) + (mm(a[0], b[1]) + mm(a[1], b[0]))


def spline_weights(t):
    square = t * t
    cube = square * t
    rest = 1.0 - t
    return [
        rest * rest * rest / 6.0,
        (3.0 * cube - 6.0 * square + 4.0) / 6.0,
        (-3.0 * cube + 3.0 * square + 3.0 * t + 1.0) / 6.0,
        cube / 6.0,
    ]


def line_weights(start, weights, dim):
    rows = lax.broadcasted_iota(jnp.int32, (128, start.shape[1]), 0)
    at = (rows - start[dim : dim + 1]) & 127
    result = jnp.zeros(at.shape, F32)
    for j in range(4):
        result = jnp.where(at == j, weights[j][dim : dim + 1], result)
    return result


def plane_weights(start, weights, planes):
    offset = start[0:1] & 3
    result = []
    for plane in planes:
        total = jnp.zeros(offset.shape, F32)
        for j in range(4):
            total = jnp.where(offset + j == plane, weights[j][0:1], total)
        result.append(total)
    return result


def swap_blocks(a):
    lane = lax.broadcasted_iota(jnp.int32, a[0].shape, 1)
    wide = lane < 64
    narrow = (lane & 63) < 32
    b = [None] * 4
    for i in range(2):
        b[i] = jnp.where(wide, a[i], pltpu.roll(a[i + 2], 64, 1))
        b[i + 2] = jnp.where(wide, pltpu.roll(a[i], 64, 1), a[i + 2])
    o = [None] * 4
    for i in (0, 2):
        o[i] = jnp.where(narrow, b[i], pltpu.roll(b[i + 1], 32, 1))
        o[i + 1] = jnp.where(narrow, pltpu.roll(b[i], 96, 1), b[i + 1])
    return o


def prepare(start_ref, fraction_ref, table, y_pair, z_modes, along, planes):
    def step(k, carry):
        cols = pl.ds(pl.multiple_of(k * 256, 256), 256)
        start = start_ref[:, cols]
        weights = spline_weights(fraction_ref[:, cols])
        y_high, y_low = split(line_weights(start, weights, 1))
        y_pair[:128, cols] = y_high
        y_pair[128:, cols] = y_low
        z_modes[:, cols] = mm3(table, split(line_weights(start, weights, 2)))
        for i, row in enumerate(plane_weights(start, weights, planes)):
            along[i : i + 1, cols] = row
        return carry

    lax.fori_loop(0, start_ref.shape[1] // 256, step, 0, unroll=2)


def back_modes(start_ref, fraction_ref, table, z_modes):
    def step(k, carry):
        cols = pl.ds(pl.multiple_of(k * 256, 256), 256)
        weights = spline_weights(fraction_ref[:, cols])
        z_modes[:, cols] = mm3(table, split(line_weights(start_ref[:, cols], weights, 2)))
        return carry

    lax.fori_loop(0, start_ref.shape[1] // 256, step, 0, unroll=2)


def spread(c, count, force_ref, y_pair, z_modes, along, acc):
    def step(k, carry):
        cols = pl.ds(pl.multiple_of(k * CHUNK, CHUNK), CHUNK)
        z = z_modes[:, cols]
        right = y_pair[:, cols]
        force = force_ref[c : c + 1, cols]
        pieces = [split(z * (force * along[i : i + 1, cols])) for i in range(count)]
        high = jnp.concatenate([p[0] for p in pieces], axis=0)
        low = jnp.concatenate([p[1] for p in pieces], axis=0)
        dims = (((1,), (1,)), ((), ()))
        acc[c, : count * 128, :] += lax.dot_general(
            high, right, dims, preferred_element_type=F32
        ) + lax.dot_general(low, right, dims, preferred_element_type=F32)
        return carry

    lax.fori_loop(0, force_ref.shape[1] // CHUNK, step, 0)


def gather(c, count, y_pair, z_modes, along, left, out):
    def step(k, carry):
        cols = pl.ds(pl.multiple_of(k * CHUNK, CHUNK), CHUNK)
        pair = y_pair[:, cols]
        twice = jnp.concatenate([pair[:128], pair[:128]], axis=0)
        both = left[c, : count * 128, :]
        value = mm(both, twice) + mm(both[:, :128], pair[128:])
        total = value[:128] * along[0:1, cols]
        for i in range(1, count):
            total = total + value[i * 128 : i * 128 + 128] * along[i : i + 1, cols]
        out[c : c + 1, cols] = jnp.sum(total * z_modes[:, cols], axis=0, keepdims=True)
        return carry

    lax.fori_loop(0, out.shape[1] // CHUNK, step, 0)


def lines_forward(acc, c, table, send):
    parts = []
    for x in range(4):
        rows = pl.ds(x * 128, 128)
        value = mm3(split(acc[c, rows, :128] + acc[c, rows, 128:]), table)
        re, im = value[:64], value[64:]
        parts.append((re[:, :128] + im[:, 128:], im[:, :128] - re[:, 128:]))
    for part in range(2):
        blocks = swap_blocks([p[part] for p in parts])
        for q in range(4):
            send[c, pl.ds(q * 128 + part, 64, stride=2), :] = blocks[q]


def lines_back(lines, c, table, left):
    parts = []
    for part in range(2):
        parts.append(swap_blocks([lines[c, pl.ds(q * 128 + part, 64, stride=2), :] for q in range(4)]))
    for x in range(4):
        value = mm3(split(jnp.concatenate([parts[0][x], parts[1][x]], axis=0)), table)
        re, im = value[:64], value[64:]
        plane = jnp.concatenate([re[:, :128] - im[:, 128:], im[:, :128] + re[:, 128:]], axis=0)
        left[c, pl.ds(x * 128, 128), :] = jnp.concatenate(split(plane), axis=1)


def pick_tiles(ends, start_ref, fraction_ref, force_ref, by_tile, tiles):
    count = start_ref.shape[1] // 128
    flat = by_tile.reshape(count * 16, 128)
    for t in range(count):
        cols = slice(t * 128, t * 128 + 128)
        by_tile[t, 0:3, :] = start_ref[:, cols].astype(F32)
        by_tile[t, 3:6, :] = fraction_ref[:, cols]
        by_tile[t, 6:9, :] = force_ref[:, cols]
    target = tiles.reshape(2 * SLOTS * 16, 128)
    for k in range(9):
        target[pl.ds(k, 2 * SLOTS, stride=16), :] = lax.dot_general(
            ends,
            flat[pl.ds(k, count, stride=16), :],
            (((0,), (0,)), ((), ())),
            precision=lax.Precision.HIGHEST,
            preferred_element_type=F32,
        )


def near_sum(live, terms, near):
    for c in range(3):
        value = jnp.dot(live, terms[c], precision=lax.Precision.HIGHEST, preferred_element_type=F32)
        for t in range(value.shape[0]):
            near[c : c + 1, t * 128 : t * 128 + 128] = value[t : t + 1]


def near_terms(tiles, terms, first, last):
    def slot(s, carry):
        row = tiles[s]
        col = tiles[SLOTS + s].T
        gap = []
        for d in range(3):
            whole_gap = row[d : d + 1] - col[:, d : d + 1]
            if d > 0:
                whole_gap = jnp.where(whole_gap > 64.0, whole_gap - 128.0, whole_gap)
                whole_gap = jnp.where(whole_gap < -64.0, whole_gap + 128.0, whole_gap)
            gap.append(whole_gap + (row[3 + d : 4 + d] - col[:, 3 + d : 4 + d]))
        distance = gap[0] * gap[0] + gap[1] * gap[1] + gap[2] * gap[2]
        inverse = lax.rsqrt(distance + 1.0)
        fall = jnp.exp2(distance * (-0.0625 * LOG2_E)) * (0.25 * inverse * inverse * inverse)
        pulled = [col[:, 6 + c : 7 + c] for c in range(3)]
        along = (gap[0] * pulled[0] + gap[1] * pulled[1] + gap[2] * pulled[2]) * fall
        diagonal = (distance + 2.0) * fall
        for c in range(3):
            term = diagonal * pulled[c] + along * gap[c]
            terms[c, pl.ds(s, 1), :] = jnp.sum(term, axis=0, keepdims=True)
        return carry

    lax.fori_loop(first, last, slot, 0, unroll=2)


def step_kernel(
    start, fraction, force, pairs, used, fz_high, fz_low, bz_high, bz_low, ty_high, ty_low,
    fx_high_far, fx_low_far, mix_far, unmix_far, cos_far, sin_far,
    out, partial_in,
    start_b, fraction_b, force_b, y_pair, z_modes, along, acc, left, by_tile, tiles, terms, near,
    fx_high, fx_low, mix, unmix, turn_cos, turn_sin, bx_high, bx_low,
    send, mid_a, held, back, mid_b, lines, modes, partial,
    send_sem, recv_sem, local_sem, table_sem, point_send, point_recv, last_send, last_recv,
):
    me = lax.axis_index("group") * 128 + lax.axis_index("dev")
    yx = me >> 4
    zc = me & 15

    def at(yx_, zc_):
        index = yx_ * 16 + zc_
        return (index >> 7, index & 127)

    def near_by(by):
        index = (me + by) & 255
        return (index >> 7, index & 127)

    barrier = pltpu.get_barrier_semaphore()
    for by in (1, 255):
        pl.semaphore_signal(barrier, inc=1, device_id=near_by(by), device_id_type=MESH)
    for j in range(1, 16):
        pl.semaphore_signal(barrier, inc=1, device_id=at(yx, (zc + j) & 15), device_id_type=MESH)
        pl.semaphore_signal(barrier, inc=1, device_id=at((yx + j) & 15, zc), device_id_type=MESH)

    table_copies = [
        pltpu.make_async_copy(source, target, table_sem.at[i])
        for i, (source, target) in enumerate(
            [
                (fx_high_far, fx_high), (fx_low_far, fx_low),
                (mix_far, mix), (unmix_far, unmix), (cos_far, turn_cos), (sin_far, turn_sin),
            ]
        )
    ]
    for copy in table_copies:
        copy.start()

    shape = (3, 16, 16, 2, 128)
    send_blocks, back_blocks, lines_blocks = send.reshape(shape), back.reshape(shape), lines.reshape(shape)
    most = pl.ds(0, 15)

    def phase(number, c, source, target, along_z):
        here = zc if along_z else yx
        pltpu.make_async_copy(source(here), target, local_sem.at[number, c]).start()
        for j in range(1, 16):
            there = (here + j) & 15
            pltpu.make_async_remote_copy(
                src_ref=source(there),
                dst_ref=target,
                send_sem=send_sem.at[number, c],
                recv_sem=recv_sem.at[number, c],
                device_id=at(yx, there) if along_z else at(there, zc),
                device_id_type=MESH,
            ).start()

    def finish(number, c, source, target, whole_source, whole_target):
        pltpu.make_async_copy(source, target, local_sem.at[number, c]).wait()
        everything = pltpu.make_async_remote_copy(
            src_ref=whole_source,
            dst_ref=whole_target,
            send_sem=send_sem.at[number, c],
            recv_sem=recv_sem.at[number, c],
            device_id=near_by(1),
            device_id_type=MESH,
        )
        everything.wait_recv()
        everything.wait_send()

    table_z = (fz_high[...], fz_low[...])
    table_y = (ty_high[...], ty_low[...])
    y_own, z_own, a_own = y_pair.at[0], z_modes.at[0], along.at[0]
    y_behind, z_behind, a_behind = y_pair.at[1], z_modes.at[1], along.at[1]

    pl.semaphore_wait(barrier, 32)
    points = [
        pltpu.make_async_remote_copy(
            src_ref=source,
            dst_ref=target,
            send_sem=point_send.at[i],
            recv_sem=point_recv.at[i],
            device_id=near_by(1),
            device_id_type=MESH,
        )
        for i, (source, target) in enumerate([(start, start_b), (fraction, fraction_b), (force, force_b)])
    ]
    for copy in points:
        copy.start()
    acc[...] = jnp.zeros_like(acc)
    prepare(start, fraction, table_z, y_own, z_own, a_own, range(4))
    spread(0, 4, force, y_own, z_own, a_own, acc)
    for copy in points:
        copy.wait()
    prepare(start_b, fraction_b, table_z, y_behind, z_behind, a_behind, range(4, 7))
    for c in range(3):
        if c > 0:
            spread(c, 4, force, y_own, z_own, a_own, acc)
        spread(c, 3, force_b, y_behind, z_behind, a_behind, acc)
        lines_forward(acc, c, table_y, send)
        phase(0, c, lambda z, c=c: send_blocks.at[c, z], mid_a.at[c, zc], True)

    def half_way(c):
        finish(0, c, send_blocks.at[c, zc], mid_a.at[c, zc], send_blocks.at[c, most], mid_a.at[c, most])
        phase(1, c, lambda y, c=c: mid_a.at[c, :, y], held.at[c, yx], False)

    def line_modes(c):
        finish(1, c, mid_a.at[c, :, yx], held.at[c, yx], held.at[c, most], held.at[c, most])
        value = split(held.reshape(3, 512, 128)[c])
        both = jnp.concatenate(value, axis=1)
        top = mm(fx_high[...], both)
        value = top[:, :128] + (top[:, 128:] + mm(fx_low[...], value[0]))
        re, im = value[:256], value[256:]
        cos, sin = turn_cos[...], turn_sin[...]
        turned = jnp.concatenate([re * cos + im * sin, im * cos - re * sin], axis=1)
        high, low = split(turned)
        modes[c] = mm(high, mix[...]) + mm(low, mix[...])

    half_way(0)
    slot_tile = lax.broadcasted_iota(jnp.int32, (start.shape[1] // 128, SLOTS), 0)
    ends = jnp.concatenate([jnp.where(slot_tile == pairs[e : e + 1, :], 1.0, 0.0) for e in range(2)], axis=1)
    pick_tiles(ends, start, fraction, force, by_tile, tiles)
    for copy in table_copies:
        copy.wait()
    bx_high[...] = fx_high[...].T
    bx_low[...] = fx_low[...].T
    near_terms(tiles, terms, 0, 12)
    half_way(1)
    line_modes(0)
    back_modes(start, fraction, (bz_high[...], bz_low[...]), z_own)
    back_modes(start_b, fraction_b, (bz_high[...], bz_low[...]), z_behind)
    near_terms(tiles, terms, 12, 16)
    half_way(2)
    line_modes(1)
    line_modes(2)

    column = zc * 16 + yx
    lane = lax.broadcasted_iota(jnp.int32, (256, 128), 1)
    row = lax.broadcasted_iota(jnp.int32, (256, 128), 0)
    index_x = row + 256 * (lane >> 5)
    index_y = (lane & 31) + 32 * (column >> 6)
    index_z = column & 63
    step_x = TWO_PI / NX
    step_y = TWO_PI / NY
    wave_x = jnp.where(index_x > 512, index_x - 1024, index_x).astype(F32) * step_x
    wave_y = jnp.where(index_y > 64, index_y - 128, index_y).astype(F32) * step_y
    wave_z = index_z.astype(F32) * step_y
    squared = wave_x * wave_x + wave_y * wave_y + wave_z * wave_z
    anchor = squared == 0.0
    drop = anchor | (index_x == 512) | (index_y == 64)
    inverse = jnp.where(drop, 0.0, 1.0 / jnp.where(anchor, 1.0, squared))
    waves = (wave_x, wave_y, wave_z)
    for part in range(2):
        lanes = slice(part * 128, part * 128 + 128)
        values = [modes[c, :, lanes] for c in range(3)]
        project = (wave_x * values[0] + wave_y * values[1] + wave_z * values[2]) * inverse
        for c in range(3):
            modes[c, :, lanes] = (values[c] - waves[c] * project) * inverse

    def way_back(c):
        high, low = split(modes[c])
        value = mm(high, unmix[...]) + mm(low, unmix[...])
        re, im = value[:, :128], value[:, 128:]
        cos, sin = turn_cos[...], turn_sin[...]
        value = split(jnp.concatenate([re * cos - im * sin, im * cos + re * sin], axis=0))
        both = jnp.concatenate(value, axis=1)
        top = mm(bx_high[...], both)
        back[c] = top[:, :128] + (top[:, 128:] + mm(bx_low[...], value[0]))
        phase(2, c, lambda y: back_blocks.at[c, y], mid_b.at[c, yx], False)

    def last_way(c):
        finish(2, c, back_blocks.at[c, yx], mid_b.at[c, yx], back_blocks.at[c, most], mid_b.at[c, most])
        phase(3, c, lambda z: mid_b.at[c, :, z], lines_blocks.at[c, zc], True)

    way_back(0)
    way_back(1)
    last_way(0)
    way_back(2)
    near_terms(tiles, terms, 16, 26)
    last_way(1)
    near_terms(tiles, terms, 26, 36)
    last_way(2)
    near_terms(tiles, terms, 36, SLOTS)
    slot = lax.broadcasted_iota(jnp.int32, slot_tile.shape, 1)
    live = jnp.where((slot_tile == pairs[0:1, :]) & (slot < used[0]), 1.0, 0.0)
    near_sum(live, terms, near)

    last = pltpu.make_async_remote_copy(
        src_ref=partial,
        dst_ref=partial_in,
        send_sem=last_send,
        recv_sem=last_recv,
        device_id=near_by(255),
        device_id_type=MESH,
    )
    for c in range(3):
        finish(3, c, mid_b.at[c, :, zc], lines_blocks.at[c, zc], lines_blocks.at[c, most], lines_blocks.at[c, most])
        lines_back(lines, c, table_y, left)
        gather(c, 3, y_behind, z_behind, a_behind, left, partial)
        if c == 2:
            last.start()
        gather(c, 4, y_own, z_own, a_own, left, out)
    last.wait()
    out[...] = out[...] + near[...]


def step(forces, stencil_start, fraction, tile_pairs, pair_count, tables):
    count = forces.shape[1]
    vmem = pl.BlockSpec(memory_space=pltpu.VMEM)
    far = pl.BlockSpec(memory_space=pl.ANY)
    blocks = (3, 16, 16, 2, 128)
    x_tables = [*tables["forward_x"], tables["mix"], tables["unmix"], *tables["turn"]]
    dma = pltpu.SemaphoreType.DMA
    return pl.pallas_call(
        step_kernel,
        in_specs=[vmem] * 4 + [pl.BlockSpec(memory_space=pltpu.SMEM)] + [vmem] * 6 + [far] * 6,
        out_specs=[vmem, vmem],
        out_shape=[jax.ShapeDtypeStruct((3, count), F32)] * 2,
        scratch_shapes=[
            VMEM((3, count), jnp.int32),
            VMEM((3, count), F32),
            VMEM((3, count), F32),
            VMEM((2, 256, count), BF16),
            VMEM((2, 128, count), F32),
            VMEM((2, 8, count), F32),
            VMEM((3, 512, 256), F32),
            VMEM((3, 512, 256), BF16),
            VMEM((count // 128, 16, 128), F32),
            VMEM((2 * SLOTS, 16, 128), F32),
            VMEM((3, SLOTS, 128), F32),
            VMEM((3, count), F32),
        ]
        + [VMEM(t.shape, t.dtype) for t in x_tables]
        + [VMEM((512, 512), BF16)] * 2
        + [
            VMEM((3, 512, 128), F32),
            VMEM(blocks, F32),
            VMEM(blocks, F32),
            VMEM((3, 512, 128), F32),
            VMEM(blocks, F32),
            VMEM((3, 512, 128), F32),
            VMEM((3, 256, 256), F32),
            VMEM((3, count), F32),
            dma((4, 3)),
            dma((4, 3)),
            dma((4, 3)),
            dma((6,)),
            dma((3,)),
            dma((3,)),
            dma,
            dma,
        ],
        compiler_params=pltpu.CompilerParams(collective_id=0, has_side_effects=True),
        name="step",
    )(
        stencil_start,
        fraction,
        forces,
        tile_pairs.T,
        pair_count,
        *tables["forward_z"],
        *tables["back_z"],
        *tables["table_y"],
        *x_tables,
    )


def per_device(tables, forces, stencil_start, fraction, tile_pairs, pair_count):
    far, behind = step(forces, stencil_start, fraction, tile_pairs, pair_count, tables)
    return far + behind


def solution(mesh):
    tables = make_tables()
    in_specs = (
        P(None, ("group", "dev")),
        P(None, ("group", "dev")),
        P(None, ("group", "dev")),
        P(("group", "dev"), None),
        P(("group", "dev")),
    )
    return jax.shard_map(
        functools.partial(per_device, tables),
        mesh=mesh,
        in_specs=in_specs,
        out_specs=P(None, ("group", "dev")),
        check_vma=False,
    )
```

```python
import functools

import jax
import jax.numpy as jnp
import numpy as np
from jax import lax
from jax.experimental import pallas as pl
from jax.experimental.pallas import tpu as pltpu
from jax.sharding import PartitionSpec as P

NX = 1024
NY = 128
NZ = 128
MESH = pl.DeviceIdType.MESH
F32 = jnp.float32
BF16 = jnp.bfloat16
TWO_PI = 2.0 * np.pi
CHUNK = 512
VMEM = pltpu.VMEM
SLOTS = 48
LOG2_E = 1.4426950408889634


def halves(table):
    table = np.asarray(table, np.float32)
    high = table.astype(BF16)
    low = (table - high.astype(np.float32)).astype(BF16)
    return jnp.asarray(high), jnp.asarray(low)


def make_tables():
    k = np.arange(64)[:, None]
    z = np.arange(128)[None, :]
    angle = TWO_PI * ((k * z) % 128) / 128
    forward_z = np.concatenate([np.cos(angle), -np.sin(angle)], 0)
    weight = np.where(k == 0, 1.0, 2.0) / float(NX * NY * NZ)
    back_z = np.concatenate([weight * np.cos(angle), -weight * np.sin(angle)], 0)
    n = np.arange(128)
    angle = TWO_PI * ((n[:, None] * n[None, :]) % 128) / 128
    table_y = np.concatenate([np.cos(angle), np.sin(angle)], 1)
    n = np.arange(256)
    angle = TWO_PI * ((n[:, None] * n[None, :]) % 256) / 256
    cosine, sine = np.cos(angle), np.sin(angle)
    forward_x = np.zeros((2, 256, 256, 2))
    forward_x[0, :, :, 0] = cosine
    forward_x[0, :, :, 1] = sine
    forward_x[1, :, :, 0] = -sine
    forward_x[1, :, :, 1] = cosine
    forward_x = forward_x.reshape(512, 512)
    mix = np.zeros((2, 4, 32, 2, 4, 32))
    for r in range(4):
        for x in range(4):
            factor = (-1j) ** (r * x)
            for lane in range(32):
                mix[0, x, lane, 0, r, lane] = round(factor.real)
                mix[0, x, lane, 1, r, lane] = round(factor.imag)
                mix[1, x, lane, 0, r, lane] = -round(factor.imag)
                mix[1, x, lane, 1, r, lane] = round(factor.real)
    mix = mix.reshape(256, 256)
    q = np.arange(256)[:, None]
    x = (np.arange(128) // 32)[None, :]
    angle = TWO_PI * ((q * x) % 1024) / 1024
    return dict(
        forward_z=halves(forward_z),
        back_z=halves(back_z),
        table_y=halves(table_y),
        forward_x=halves(forward_x),
        mix=jnp.asarray(mix.astype(BF16)),
        unmix=jnp.asarray(mix.T.astype(BF16)),
        turn=(jnp.asarray(np.cos(angle).astype(np.float32)), jnp.asarray(np.sin(angle).astype(np.float32))),
    )


def split(value):
    high = value.astype(BF16)
    low = (value - high.astype(F32)).astype(BF16)
    return high, low


def mm(a, b):
    return jnp.dot(a, b, preferred_element_type=F32)


def mm3(a, b):
    return mm(a[0], b[0]) + (mm(a[0], b[1]) + mm(a[1], b[0]))


def spline_weights(t):
    square = t * t
    cube = square * t
    rest = 1.0 - t
    return [
        rest * rest * rest / 6.0,
        (3.0 * cube - 6.0 * square + 4.0) / 6.0,
        (-3.0 * cube + 3.0 * square + 3.0 * t + 1.0) / 6.0,
        cube / 6.0,
    ]


def line_weights(start, weights, dim):
    rows = lax.broadcasted_iota(jnp.int32, (128, start.shape[1]), 0)
    at = (rows - start[dim : dim + 1]) & 127
    result = jnp.zeros(at.shape, F32)
    for j in range(4):
        result = jnp.where(at == j, weights[j][dim : dim + 1], result)
    return result


def plane_weights(start, weights, planes):
    offset = start[0:1] & 3
    result = []
    for plane in planes:
        total = jnp.zeros(offset.shape, F32)
        for j in range(4):
            total = jnp.where(offset + j == plane, weights[j][0:1], total)
        result.append(total)
    return result


def swap_blocks(a):
    lane = lax.broadcasted_iota(jnp.int32, a[0].shape, 1)
    wide = lane < 64
    narrow = (lane & 63) < 32
    b = [None] * 4
    for i in range(2):
        b[i] = jnp.where(wide, a[i], pltpu.roll(a[i + 2], 64, 1))
        b[i + 2] = jnp.where(wide, pltpu.roll(a[i], 64, 1), a[i + 2])
    o = [None] * 4
    for i in (0, 2):
        o[i] = jnp.where(narrow, b[i], pltpu.roll(b[i + 1], 32, 1))
        o[i + 1] = jnp.where(narrow, pltpu.roll(b[i], 96, 1), b[i + 1])
    return o


def prepare(start_ref, fraction_ref, table, y_pair, z_modes, along, planes):
    def step(k, carry):
        cols = pl.ds(pl.multiple_of(k * 256, 256), 256)
        start = start_ref[:, cols]
        weights = spline_weights(fraction_ref[:, cols])
        y_high, y_low = split(line_weights(start, weights, 1))
        y_pair[:128, cols] = y_high
        y_pair[128:, cols] = y_low
        z_modes[:, cols] = mm3(table, split(line_weights(start, weights, 2)))
        for i, row in enumerate(plane_weights(start, weights, planes)):
            along[i : i + 1, cols] = row
        return carry

    lax.fori_loop(0, start_ref.shape[1] // 256, step, 0, unroll=2)


def back_modes(start_ref, fraction_ref, table, z_modes):
    def step(k, carry):
        cols = pl.ds(pl.multiple_of(k * 256, 256), 256)
        weights = spline_weights(fraction_ref[:, cols])
        z_modes[:, cols] = mm3(table, split(line_weights(start_ref[:, cols], weights, 2)))
        return carry

    lax.fori_loop(0, start_ref.shape[1] // 256, step, 0, unroll=2)


def spread(c, count, force_ref, y_pair, z_modes, along, acc):
    def step(k, carry):
        cols = pl.ds(pl.multiple_of(k * CHUNK, CHUNK), CHUNK)
        z = z_modes[:, cols]
        right = y_pair[:, cols]
        force = force_ref[c : c + 1, cols]
        pieces = [split(z * (force * along[i : i + 1, cols])) for i in range(count)]
        high = jnp.concatenate([p[0] for p in pieces], axis=0)
        low = jnp.concatenate([p[1] for p in pieces], axis=0)
        dims = (((1,), (1,)), ((), ()))
        acc[c, : count * 128, :] += lax.dot_general(
            high, right, dims, preferred_element_type=F32
        ) + lax.dot_general(low, right, dims, preferred_element_type=F32)
        return carry

    lax.fori_loop(0, force_ref.shape[1] // CHUNK, step, 0, unroll=2)


def gather(c, count, y_pair, z_modes, along, left, out):
    def step(k, carry):
        cols = pl.ds(pl.multiple_of(k * CHUNK, CHUNK), CHUNK)
        pair = y_pair[:, cols]
        twice = jnp.concatenate([pair[:128], pair[:128]], axis=0)
        both = left[c, : count * 128, :]
        value = mm(both, twice) + mm(both[:, :128], pair[128:])
        total = value[:128] * along[0:1, cols]
        for i in range(1, count):
            total = total + value[i * 128 : i * 128 + 128] * along[i : i + 1, cols]
        out[c : c + 1, cols] = jnp.sum(total * z_modes[:, cols], axis=0, keepdims=True)
        return carry

    lax.fori_loop(0, out.shape[1] // CHUNK, step, 0, unroll=2)


def lines_forward(acc, c, table, send):
    parts = []
    for x in range(4):
        rows = pl.ds(x * 128, 128)
        value = mm3(split(acc[c, rows, :128] + acc[c, rows, 128:]), table)
        re, im = value[:64], value[64:]
        parts.append((re[:, :128] + im[:, 128:], im[:, :128] - re[:, 128:]))
    for part in range(2):
        blocks = swap_blocks([p[part] for p in parts])
        for q in range(4):
            send[c, pl.ds(q * 128 + part, 64, stride=2), :] = blocks[q]


def lines_back(lines, c, table, left):
    parts = []
    for part in range(2):
        parts.append(swap_blocks([lines[c, pl.ds(q * 128 + part, 64, stride=2), :] for q in range(4)]))
    for x in range(4):
        value = mm3(split(jnp.concatenate([parts[0][x], parts[1][x]], axis=0)), table)
        re, im = value[:64], value[64:]
        plane = jnp.concatenate([re[:, :128] - im[:, 128:], im[:, :128] + re[:, 128:]], axis=0)
        left[c, pl.ds(x * 128, 128), :] = jnp.concatenate(split(plane), axis=1)


def pick_tiles(ends, start_ref, fraction_ref, force_ref, by_tile, tiles):
    count = start_ref.shape[1] // 128
    flat = by_tile.reshape(count * 16, 128)
    for t in range(count):
        cols = slice(t * 128, t * 128 + 128)
        by_tile[t, 0:3, :] = start_ref[:, cols].astype(F32)
        by_tile[t, 3:6, :] = fraction_ref[:, cols]
        by_tile[t, 6:9, :] = force_ref[:, cols]
    target = tiles.reshape(2 * SLOTS * 16, 128)
    for k in range(9):
        target[pl.ds(k, 2 * SLOTS, stride=16), :] = lax.dot_general(
            ends,
            flat[pl.ds(k, count, stride=16), :],
            (((0,), (0,)), ((), ())),
            precision=lax.Precision.HIGHEST,
            preferred_element_type=F32,
        )


def near_sum(live, terms, near):
    for c in range(3):
        value = jnp.dot(live, terms[c], precision=lax.Precision.HIGHEST, preferred_element_type=F32)
        for t in range(value.shape[0]):
            near[c : c + 1, t * 128 : t * 128 + 128] = value[t : t + 1]


def near_terms(tiles, terms, first, last):
    def slot(s, carry):
        row = tiles[s]
        col = tiles[SLOTS + s].T
        gap = []
        for d in range(3):
            whole_gap = row[d : d + 1] - col[:, d : d + 1]
            if d > 0:
                whole_gap = whole_gap - 128.0 * jnp.round(whole_gap * (1.0 / 128.0))
            gap.append(whole_gap + (row[3 + d : 4 + d] - col[:, 3 + d : 4 + d]))
        distance = gap[0] * gap[0] + gap[1] * gap[1] + gap[2] * gap[2]
        inverse = lax.rsqrt(distance + 1.0)
        fall = jnp.exp2(distance * (-0.0625 * LOG2_E)) * (0.25 * inverse * inverse * inverse)
        pulled = [col[:, 6 + c : 7 + c] for c in range(3)]
        along = (gap[0] * pulled[0] + gap[1] * pulled[1] + gap[2] * pulled[2]) * fall
        diagonal = (distance + 2.0) * fall
        for c in range(3):
            term = diagonal * pulled[c] + along * gap[c]
            terms[c, pl.ds(s, 1), :] = jnp.sum(term, axis=0, keepdims=True)
        return carry

    lax.fori_loop(first, last, slot, 0, unroll=2)


def step_kernel(
    start, fraction, force, pairs, used, fz_high, fz_low, bz_high, bz_low, ty_high, ty_low,
    fx_high_far, fx_low_far, mix_far, unmix_far, cos_far, sin_far,
    out, partial_in,
    start_b, fraction_b, force_b, y_pair, z_modes, along, acc, left, by_tile, tiles, terms, near,
    fx_high, fx_low, mix, unmix, turn_cos, turn_sin, bx_high, bx_low,
    send, mid_a, held, back, mid_b, lines, modes, partial,
    send_sem, recv_sem, local_sem, table_sem, point_send, point_recv, last_send, last_recv,
):
    me = lax.axis_index("group") * 128 + lax.axis_index("dev")
    yx = me >> 4
    zc = me & 15

    def at(yx_, zc_):
        index = yx_ * 16 + zc_
        return (index >> 7, index & 127)

    def near_by(by):
        index = (me + by) & 255
        return (index >> 7, index & 127)

    barrier = pltpu.get_barrier_semaphore()
    for by in (1, 255):
        pl.semaphore_signal(barrier, inc=1, device_id=near_by(by), device_id_type=MESH)
    for j in range(1, 16):
        pl.semaphore_signal(barrier, inc=1, device_id=at(yx, (zc + j) & 15), device_id_type=MESH)
        pl.semaphore_signal(barrier, inc=1, device_id=at((yx + j) & 15, zc), device_id_type=MESH)

    table_copies = [
        pltpu.make_async_copy(source, target, table_sem.at[i])
        for i, (source, target) in enumerate(
            [
                (fx_high_far, fx_high), (fx_low_far, fx_low),
                (mix_far, mix), (unmix_far, unmix), (cos_far, turn_cos), (sin_far, turn_sin),
            ]
        )
    ]
    for copy in table_copies:
        copy.start()

    shape = (3, 16, 16, 2, 128)
    send_blocks, back_blocks, lines_blocks = send.reshape(shape), back.reshape(shape), lines.reshape(shape)
    most = pl.ds(0, 15)

    def phase(number, c, source, target, along_z):
        here = zc if along_z else yx
        pltpu.make_async_copy(source(here), target, local_sem.at[number, c]).start()
        for j in range(1, 16):
            there = (here + j) & 15
            pltpu.make_async_remote_copy(
                src_ref=source(there),
                dst_ref=target,
                send_sem=send_sem.at[number, c],
                recv_sem=recv_sem.at[number, c],
                device_id=at(yx, there) if along_z else at(there, zc),
                device_id_type=MESH,
            ).start()

    def finish(number, c, source, target, whole_source, whole_target):
        pltpu.make_async_copy(source, target, local_sem.at[number, c]).wait()
        everything = pltpu.make_async_remote_copy(
            src_ref=whole_source,
            dst_ref=whole_target,
            send_sem=send_sem.at[number, c],
            recv_sem=recv_sem.at[number, c],
            device_id=near_by(1),
            device_id_type=MESH,
        )
        everything.wait_recv()
        everything.wait_send()

    table_z = (fz_high[...], fz_low[...])
    table_y = (ty_high[...], ty_low[...])
    y_own, z_own, a_own = y_pair.at[0], z_modes.at[0], along.at[0]
    y_behind, z_behind, a_behind = y_pair.at[1], z_modes.at[1], along.at[1]

    pl.semaphore_wait(barrier, 32)
    points = [
        pltpu.make_async_remote_copy(
            src_ref=source,
            dst_ref=target,
            send_sem=point_send.at[i],
            recv_sem=point_recv.at[i],
            device_id=near_by(1),
            device_id_type=MESH,
        )
        for i, (source, target) in enumerate([(start, start_b), (fraction, fraction_b), (force, force_b)])
    ]
    for copy in points:
        copy.start()
    acc[...] = jnp.zeros_like(acc)
    prepare(start, fraction, table_z, y_own, z_own, a_own, range(4))
    spread(0, 4, force, y_own, z_own, a_own, acc)
    for copy in points:
        copy.wait()
    prepare(start_b, fraction_b, table_z, y_behind, z_behind, a_behind, range(4, 7))
    for c in range(3):
        if c > 0:
            spread(c, 4, force, y_own, z_own, a_own, acc)
        spread(c, 3, force_b, y_behind, z_behind, a_behind, acc)
        lines_forward(acc, c, table_y, send)
        phase(0, c, lambda z, c=c: send_blocks.at[c, z], mid_a.at[c, zc], True)

    def half_way(c):
        finish(0, c, send_blocks.at[c, zc], mid_a.at[c, zc], send_blocks.at[c, most], mid_a.at[c, most])
        phase(1, c, lambda y, c=c: mid_a.at[c, :, y], held.at[c, yx], False)

    def line_modes(c):
        finish(1, c, mid_a.at[c, :, yx], held.at[c, yx], held.at[c, most], held.at[c, most])
        value = split(held.reshape(3, 512, 128)[c])
        both = jnp.concatenate(value, axis=1)
        top = mm(fx_high[...], both)
        value = top[:, :128] + (top[:, 128:] + mm(fx_low[...], value[0]))
        re, im = value[:256], value[256:]
        cos, sin = turn_cos[...], turn_sin[...]
        turned = jnp.concatenate([re * cos + im * sin, im * cos - re * sin], axis=1)
        high, low = split(turned)
        modes[c] = mm(high, mix[...]) + mm(low, mix[...])

    half_way(0)
    slot_tile = lax.broadcasted_iota(jnp.int32, (start.shape[1] // 128, SLOTS), 0)
    ends = jnp.concatenate([jnp.where(slot_tile == pairs[e : e + 1, :], 1.0, 0.0) for e in range(2)], axis=1)
    pick_tiles(ends, start, fraction, force, by_tile, tiles)
    for copy in table_copies:
        copy.wait()
    bx_high[...] = fx_high[...].T
    bx_low[...] = fx_low[...].T
    near_terms(tiles, terms, 0, 12)
    half_way(1)
    line_modes(0)
    back_modes(start, fraction, (bz_high[...], bz_low[...]), z_own)
    back_modes(start_b, fraction_b, (bz_high[...], bz_low[...]), z_behind)
    near_terms(tiles, terms, 12, 16)
    half_way(2)
    line_modes(1)
    line_modes(2)

    column = zc * 16 + yx
    lane = lax.broadcasted_iota(jnp.int32, (256, 128), 1)
    row = lax.broadcasted_iota(jnp.int32, (256, 128), 0)
    index_x = row + 256 * (lane >> 5)
    index_y = (lane & 31) + 32 * (column >> 6)
    index_z = column & 63
    step_x = TWO_PI / NX
    step_y = TWO_PI / NY
    wave_x = jnp.where(index_x > 512, index_x - 1024, index_x).astype(F32) * step_x
    wave_y = jnp.where(index_y > 64, index_y - 128, index_y).astype(F32) * step_y
    wave_z = index_z.astype(F32) * step_y
    squared = wave_x * wave_x + wave_y * wave_y + wave_z * wave_z
    anchor = squared == 0.0
    drop = anchor | (index_x == 512) | (index_y == 64)
    inverse = jnp.where(drop, 0.0, 1.0 / jnp.where(anchor, 1.0, squared))
    waves = (wave_x, wave_y, wave_z)
    for part in range(2):
        lanes = slice(part * 128, part * 128 + 128)
        values = [modes[c, :, lanes] for c in range(3)]
        project = (wave_x * values[0] + wave_y * values[1] + wave_z * values[2]) * inverse
        for c in range(3):
            modes[c, :, lanes] = (values[c] - waves[c] * project) * inverse

    def way_back(c):
        high, low = split(modes[c])
        value = mm(high, unmix[...]) + mm(low, unmix[...])
        re, im = value[:, :128], value[:, 128:]
        cos, sin = turn_cos[...], turn_sin[...]
        value = split(jnp.concatenate([re * cos - im * sin, im * cos + re * sin], axis=0))
        both = jnp.concatenate(value, axis=1)
        top = mm(bx_high[...], both)
        back[c] = top[:, :128] + (top[:, 128:] + mm(bx_low[...], value[0]))
        phase(2, c, lambda y: back_blocks.at[c, y], mid_b.at[c, yx], False)

    def last_way(c):
        finish(2, c, back_blocks.at[c, yx], mid_b.at[c, yx], back_blocks.at[c, most], mid_b.at[c, most])
        phase(3, c, lambda z: mid_b.at[c, :, z], lines_blocks.at[c, zc], True)

    way_back(0)
    way_back(1)
    last_way(0)
    way_back(2)
    near_terms(tiles, terms, 16, 26)
    last_way(1)
    near_terms(tiles, terms, 26, 36)
    last_way(2)
    near_terms(tiles, terms, 36, SLOTS)
    slot = lax.broadcasted_iota(jnp.int32, slot_tile.shape, 1)
    live = jnp.where((slot_tile == pairs[0:1, :]) & (slot < used[0]), 1.0, 0.0)
    near_sum(live, terms, near)

    last = pltpu.make_async_remote_copy(
        src_ref=partial,
        dst_ref=partial_in,
        send_sem=last_send,
        recv_sem=last_recv,
        device_id=near_by(255),
        device_id_type=MESH,
    )
    for c in range(3):
        finish(3, c, mid_b.at[c, :, zc], lines_blocks.at[c, zc], lines_blocks.at[c, most], lines_blocks.at[c, most])
        lines_back(lines, c, table_y, left)
        gather(c, 3, y_behind, z_behind, a_behind, left, partial)
        if c == 2:
            last.start()
        gather(c, 4, y_own, z_own, a_own, left, out)
    last.wait()
    out[...] = out[...] + near[...]


def step(forces, stencil_start, fraction, tile_pairs, pair_count, tables):
    count = forces.shape[1]
    vmem = pl.BlockSpec(memory_space=pltpu.VMEM)
    far = pl.BlockSpec(memory_space=pl.ANY)
    blocks = (3, 16, 16, 2, 128)
    x_tables = [*tables["forward_x"], tables["mix"], tables["unmix"], *tables["turn"]]
    dma = pltpu.SemaphoreType.DMA
    return pl.pallas_call(
        step_kernel,
        in_specs=[vmem] * 4 + [pl.BlockSpec(memory_space=pltpu.SMEM)] + [vmem] * 6 + [far] * 6,
        out_specs=[vmem, vmem],
        out_shape=[jax.ShapeDtypeStruct((3, count), F32)] * 2,
        scratch_shapes=[
            VMEM((3, count), jnp.int32),
            VMEM((3, count), F32),
            VMEM((3, count), F32),
            VMEM((2, 256, count), BF16),
            VMEM((2, 128, count), F32),
            VMEM((2, 8, count), F32),
            VMEM((3, 512, 256), F32),
            VMEM((3, 512, 256), BF16),
            VMEM((count // 128, 16, 128), F32),
            VMEM((2 * SLOTS, 16, 128), F32),
            VMEM((3, SLOTS, 128), F32),
            VMEM((3, count), F32),
        ]
        + [VMEM(t.shape, t.dtype) for t in x_tables]
        + [VMEM((512, 512), BF16)] * 2
        + [
            VMEM((3, 512, 128), F32),
            VMEM(blocks, F32),
            VMEM(blocks, F32),
            VMEM((3, 512, 128), F32),
            VMEM(blocks, F32),
            VMEM((3, 512, 128), F32),
            VMEM((3, 256, 256), F32),
            VMEM((3, count), F32),
            dma((4, 3)),
            dma((4, 3)),
            dma((4, 3)),
            dma((6,)),
            dma((3,)),
            dma((3,)),
            dma,
            dma,
        ],
        compiler_params=pltpu.CompilerParams(collective_id=0, has_side_effects=True),
        name="step",
    )(
        stencil_start,
        fraction,
        forces,
        tile_pairs.T,
        pair_count,
        *tables["forward_z"],
        *tables["back_z"],
        *tables["table_y"],
        *x_tables,
    )


def per_device(tables, forces, stencil_start, fraction, tile_pairs, pair_count):
    far, behind = step(forces, stencil_start, fraction, tile_pairs, pair_count, tables)
    return far + behind


def solution(mesh):
    tables = make_tables()
    in_specs = (
        P(None, ("group", "dev")),
        P(None, ("group", "dev")),
        P(None, ("group", "dev")),
        P(("group", "dev"), None),
        P(("group", "dev")),
    )
    return jax.shard_map(
        functools.partial(per_device, tables),
        mesh=mesh,
        in_specs=in_specs,
        out_specs=P(None, ("group", "dev")),
        check_vma=False,
    )
```

```python
import functools

import jax
import jax.numpy as jnp
import numpy as np
from jax import lax
from jax.experimental import pallas as pl
from jax.experimental.pallas import tpu as pltpu
from jax.sharding import PartitionSpec as P

NX = 1024
NY = 128
NZ = 128
MESH = pl.DeviceIdType.MESH
F32 = jnp.float32
BF16 = jnp.bfloat16
TWO_PI = 2.0 * np.pi
CHUNK = 512
VMEM = pltpu.VMEM
SLOTS = 48
LOG2_E = 1.4426950408889634


def halves(table):
    table = np.asarray(table, np.float32)
    high = table.astype(BF16)
    low = (table - high.astype(np.float32)).astype(BF16)
    return jnp.asarray(high), jnp.asarray(low)


def make_tables():
    k = np.arange(64)[:, None]
    z = np.arange(128)[None, :]
    angle = TWO_PI * ((k * z) % 128) / 128
    forward_z = np.concatenate([np.cos(angle), -np.sin(angle)], 0)
    weight = np.where(k == 0, 1.0, 2.0) / float(NX * NY * NZ)
    back_z = np.concatenate([weight * np.cos(angle), -weight * np.sin(angle)], 0)
    n = np.arange(128)
    angle = TWO_PI * ((n[:, None] * n[None, :]) % 128) / 128
    table_y = np.concatenate([np.cos(angle), np.sin(angle)], 1)
    n = np.arange(256)
    angle = TWO_PI * ((n[:, None] * n[None, :]) % 256) / 256
    cosine, sine = np.cos(angle), np.sin(angle)
    forward_x = np.zeros((2, 256, 256, 2))
    forward_x[0, :, :, 0] = cosine
    forward_x[0, :, :, 1] = sine
    forward_x[1, :, :, 0] = -sine
    forward_x[1, :, :, 1] = cosine
    forward_x = forward_x.reshape(512, 512)
    mix = np.zeros((2, 4, 32, 2, 4, 32))
    for r in range(4):
        for x in range(4):
            factor = (-1j) ** (r * x)
            for lane in range(32):
                mix[0, x, lane, 0, r, lane] = round(factor.real)
                mix[0, x, lane, 1, r, lane] = round(factor.imag)
                mix[1, x, lane, 0, r, lane] = -round(factor.imag)
                mix[1, x, lane, 1, r, lane] = round(factor.real)
    mix = mix.reshape(256, 256)
    q = np.arange(256)[:, None]
    x = (np.arange(128) // 32)[None, :]
    angle = TWO_PI * ((q * x) % 1024) / 1024
    return dict(
        forward_z=halves(forward_z),
        back_z=halves(back_z),
        table_y=halves(table_y),
        forward_x=halves(forward_x),
        mix=jnp.asarray(mix.astype(BF16)),
        unmix=jnp.asarray(mix.T.astype(BF16)),
        turn=(jnp.asarray(np.cos(angle).astype(np.float32)), jnp.asarray(np.sin(angle).astype(np.float32))),
    )


def split(value):
    high = value.astype(BF16)
    low = (value - high.astype(F32)).astype(BF16)
    return high, low


def mm(a, b):
    return jnp.dot(a, b, preferred_element_type=F32)


def mm3(a, b):
    return mm(a[0], b[0]) + (mm(a[0], b[1]) + mm(a[1], b[0]))


def spline_weights(t):
    square = t * t
    cube = square * t
    rest = 1.0 - t
    return [
        rest * rest * rest / 6.0,
        (3.0 * cube - 6.0 * square + 4.0) / 6.0,
        (-3.0 * cube + 3.0 * square + 3.0 * t + 1.0) / 6.0,
        cube / 6.0,
    ]


def line_weights(start, weights, dim):
    rows = lax.broadcasted_iota(jnp.int32, (128, start.shape[1]), 0)
    at = (rows - start[dim : dim + 1]) & 127
    result = jnp.zeros(at.shape, F32)
    for j in range(4):
        result = jnp.where(at == j, weights[j][dim : dim + 1], result)
    return result


def plane_weights(start, weights, planes):
    offset = start[0:1] & 3
    result = []
    for plane in planes:
        total = jnp.zeros(offset.shape, F32)
        for j in range(4):
            total = jnp.where(offset + j == plane, weights[j][0:1], total)
        result.append(total)
    return result


def swap_blocks(a):
    lane = lax.broadcasted_iota(jnp.int32, a[0].shape, 1)
    wide = lane < 64
    narrow = (lane & 63) < 32
    b = [None] * 4
    for i in range(2):
        b[i] = jnp.where(wide, a[i], pltpu.roll(a[i + 2], 64, 1))
        b[i + 2] = jnp.where(wide, pltpu.roll(a[i], 64, 1), a[i + 2])
    o = [None] * 4
    for i in (0, 2):
        o[i] = jnp.where(narrow, b[i], pltpu.roll(b[i + 1], 32, 1))
        o[i + 1] = jnp.where(narrow, pltpu.roll(b[i], 96, 1), b[i + 1])
    return o


def prepare(start_ref, fraction_ref, table, y_pair, z_modes, along, planes):
    def step(k, carry):
        cols = pl.ds(pl.multiple_of(k * 256, 256), 256)
        start = start_ref[:, cols]
        weights = spline_weights(fraction_ref[:, cols])
        y_high, y_low = split(line_weights(start, weights, 1))
        y_pair[:128, cols] = y_high
        y_pair[128:, cols] = y_low
        z_modes[:, cols] = mm3(table, split(line_weights(start, weights, 2)))
        for i, row in enumerate(plane_weights(start, weights, planes)):
            along[i : i + 1, cols] = row
        return carry

    lax.fori_loop(0, start_ref.shape[1] // 256, step, 0, unroll=2)


def back_modes(start_ref, fraction_ref, table, z_modes):
    def step(k, carry):
        cols = pl.ds(pl.multiple_of(k * 256, 256), 256)
        weights = spline_weights(fraction_ref[:, cols])
        z_modes[:, cols] = mm3(table, split(line_weights(start_ref[:, cols], weights, 2)))
        return carry

    lax.fori_loop(0, start_ref.shape[1] // 256, step, 0, unroll=2)


def spread(c, count, force_ref, y_pair, z_modes, along, acc):
    def step(k, carry):
        cols = pl.ds(pl.multiple_of(k * CHUNK, CHUNK), CHUNK)
        z = z_modes[:, cols]
        right = y_pair[:, cols]
        force = force_ref[c : c + 1, cols]
        pieces = [split(z * (force * along[i : i + 1, cols])) for i in range(count)]
        high = jnp.concatenate([p[0] for p in pieces], axis=0)
        low = jnp.concatenate([p[1] for p in pieces], axis=0)
        dims = (((1,), (1,)), ((), ()))
        acc[c, : count * 128, :] += lax.dot_general(
            high, right, dims, preferred_element_type=F32
        ) + lax.dot_general(low, right, dims, preferred_element_type=F32)
        return carry

    lax.fori_loop(0, force_ref.shape[1] // CHUNK, step, 0, unroll=2)


def gather(c, count, y_pair, z_modes, along, left, out):
    def step(k, carry):
        cols = pl.ds(pl.multiple_of(k * CHUNK, CHUNK), CHUNK)
        pair = y_pair[:, cols]
        twice = jnp.concatenate([pair[:128], pair[:128]], axis=0)
        both = left[c, : count * 128, :]
        value = mm(both, twice) + mm(both[:, :128], pair[128:])
        total = value[:128] * along[0:1, cols]
        for i in range(1, count):
            total = total + value[i * 128 : i * 128 + 128] * along[i : i + 1, cols]
        out[c : c + 1, cols] = jnp.sum(total * z_modes[:, cols], axis=0, keepdims=True)
        return carry

    lax.fori_loop(0, out.shape[1] // CHUNK, step, 0, unroll=2)


def lines_forward(acc, c, table, send):
    parts = []
    for x in range(4):
        rows = pl.ds(x * 128, 128)
        value = mm3(split(acc[c, rows, :128] + acc[c, rows, 128:]), table)
        re, im = value[:64], value[64:]
        parts.append((re[:, :128] + im[:, 128:], im[:, :128] - re[:, 128:]))
    for part in range(2):
        blocks = swap_blocks([p[part] for p in parts])
        for q in range(4):
            send[c, pl.ds(q * 128 + part, 64, stride=2), :] = blocks[q]


def lines_back(lines, c, table, left):
    parts = []
    for part in range(2):
        parts.append(swap_blocks([lines[c, pl.ds(q * 128 + part, 64, stride=2), :] for q in range(4)]))
    for x in range(4):
        value = mm3(split(jnp.concatenate([parts[0][x], parts[1][x]], axis=0)), table)
        re, im = value[:64], value[64:]
        plane = jnp.concatenate([re[:, :128] - im[:, 128:], im[:, :128] + re[:, 128:]], axis=0)
        left[c, pl.ds(x * 128, 128), :] = jnp.concatenate(split(plane), axis=1)


def pick_tiles(ends, start_ref, fraction_ref, force_ref, by_tile, tiles):
    count = start_ref.shape[1] // 128
    flat = by_tile.reshape(count * 16, 128)
    for t in range(count):
        cols = slice(t * 128, t * 128 + 128)
        by_tile[t, 0:3, :] = start_ref[:, cols].astype(F32)
        by_tile[t, 3:6, :] = fraction_ref[:, cols]
        by_tile[t, 6:9, :] = force_ref[:, cols]
    target = tiles.reshape(2 * SLOTS * 16, 128)
    for k in range(9):
        target[pl.ds(k, 2 * SLOTS, stride=16), :] = lax.dot_general(
            ends,
            flat[pl.ds(k, count, stride=16), :],
            (((0,), (0,)), ((), ())),
            precision=lax.Precision.HIGHEST,
            preferred_element_type=F32,
        )


def near_sum(live, terms, near):
    for c in range(3):
        value = jnp.dot(live, terms[c], precision=lax.Precision.HIGHEST, preferred_element_type=F32)
        for t in range(value.shape[0]):
            near[c : c + 1, t * 128 : t * 128 + 128] = value[t : t + 1]


def near_terms(tiles, terms, first, last):
    def slot(s, carry):
        row = tiles[s]
        col = tiles[SLOTS + s].T
        gap = []
        for d in range(3):
            whole_gap = row[d : d + 1] - col[:, d : d + 1]
            if d > 0:
                whole_gap = whole_gap - 128.0 * jnp.round(whole_gap * (1.0 / 128.0))
            gap.append(whole_gap + (row[3 + d : 4 + d] - col[:, 3 + d : 4 + d]))
        distance = gap[0] * gap[0] + gap[1] * gap[1] + gap[2] * gap[2]
        inverse = lax.rsqrt(distance + 1.0)
        fall = jnp.exp2(distance * (-0.0625 * LOG2_E)) * (0.25 * inverse * inverse * inverse)
        pulled = [col[:, 6 + c : 7 + c] for c in range(3)]
        along = (gap[0] * pulled[0] + gap[1] * pulled[1] + gap[2] * pulled[2]) * fall
        diagonal = (distance + 2.0) * fall
        for c in range(3):
            term = diagonal * pulled[c] + along * gap[c]
            terms[c, pl.ds(s, 1), :] = jnp.sum(term, axis=0, keepdims=True)
        return carry

    lax.fori_loop(first, last, slot, 0, unroll=2)


def step_kernel(
    start, fraction, force, pairs, used, fz_high, fz_low, bz_high, bz_low, ty_high, ty_low,
    fx_high_far, fx_low_far, mix_far, unmix_far, cos_far, sin_far,
    out, partial_in,
    start_b, fraction_b, force_b, y_pair, z_modes, along, acc, left, by_tile, tiles, terms, near,
    fx_high, fx_low, mix, unmix, turn_cos, turn_sin, bx_high, bx_low,
    send, mid_a, held, back, mid_b, lines, modes, partial,
    send_sem, recv_sem, local_sem, table_sem, point_send, point_recv, last_send, last_recv,
):
    me = lax.axis_index("group") * 128 + lax.axis_index("dev")
    yx = me >> 4
    zc = me & 15

    def at(yx_, zc_):
        index = yx_ * 16 + zc_
        return (index >> 7, index & 127)

    def near_by(by):
        index = (me + by) & 255
        return (index >> 7, index & 127)

    barrier = pltpu.get_barrier_semaphore()
    for by in (1, 255):
        pl.semaphore_signal(barrier, inc=1, device_id=near_by(by), device_id_type=MESH)
    for j in range(1, 16):
        pl.semaphore_signal(barrier, inc=1, device_id=at(yx, (zc + j) & 15), device_id_type=MESH)
        pl.semaphore_signal(barrier, inc=1, device_id=at((yx + j) & 15, zc), device_id_type=MESH)

    table_copies = [
        pltpu.make_async_copy(source, target, table_sem.at[i])
        for i, (source, target) in enumerate(
            [
                (fx_high_far, fx_high), (fx_low_far, fx_low),
                (mix_far, mix), (unmix_far, unmix), (cos_far, turn_cos), (sin_far, turn_sin),
            ]
        )
    ]
    for copy in table_copies:
        copy.start()

    shape = (3, 16, 16, 2, 128)
    send_blocks, back_blocks, lines_blocks = send.reshape(shape), back.reshape(shape), lines.reshape(shape)
    most = pl.ds(0, 15)

    def phase(number, c, source, target, along_z):
        here = zc if along_z else yx
        pltpu.make_async_copy(source(here), target, local_sem.at[number, c]).start()
        for j in range(1, 16):
            there = (here + j) & 15
            pltpu.make_async_remote_copy(
                src_ref=source(there),
                dst_ref=target,
                send_sem=send_sem.at[number, c],
                recv_sem=recv_sem.at[number, c],
                device_id=at(yx, there) if along_z else at(there, zc),
                device_id_type=MESH,
            ).start()

    def finish(number, c, source, target, whole_source, whole_target):
        pltpu.make_async_copy(source, target, local_sem.at[number, c]).wait()
        everything = pltpu.make_async_remote_copy(
            src_ref=whole_source,
            dst_ref=whole_target,
            send_sem=send_sem.at[number, c],
            recv_sem=recv_sem.at[number, c],
            device_id=near_by(1),
            device_id_type=MESH,
        )
        everything.wait_recv()
        everything.wait_send()

    table_z = (fz_high[...], fz_low[...])
    table_y = (ty_high[...], ty_low[...])
    y_own, z_own, a_own = y_pair.at[0], z_modes.at[0], along.at[0]
    y_behind, z_behind, a_behind = y_pair.at[1], z_modes.at[1], along.at[1]

    pl.semaphore_wait(barrier, 32)
    points = [
        pltpu.make_async_remote_copy(
            src_ref=source,
            dst_ref=target,
            send_sem=point_send.at[i],
            recv_sem=point_recv.at[i],
            device_id=near_by(1),
            device_id_type=MESH,
        )
        for i, (source, target) in enumerate([(start, start_b), (fraction, fraction_b), (force, force_b)])
    ]
    for copy in points:
        copy.start()
    acc[...] = jnp.zeros_like(acc)
    prepare(start, fraction, table_z, y_own, z_own, a_own, range(4))
    spread(0, 4, force, y_own, z_own, a_own, acc)
    for copy in points:
        copy.wait()
    prepare(start_b, fraction_b, table_z, y_behind, z_behind, a_behind, range(4, 7))
    for c in range(3):
        if c > 0:
            spread(c, 4, force, y_own, z_own, a_own, acc)
        spread(c, 3, force_b, y_behind, z_behind, a_behind, acc)
        lines_forward(acc, c, table_y, send)
        phase(0, c, lambda z, c=c: send_blocks.at[c, z], mid_a.at[c, zc], True)

    def half_way(c):
        finish(0, c, send_blocks.at[c, zc], mid_a.at[c, zc], send_blocks.at[c, most], mid_a.at[c, most])
        phase(1, c, lambda y, c=c: mid_a.at[c, :, y], held.at[c, yx], False)

    def line_modes(c):
        finish(1, c, mid_a.at[c, :, yx], held.at[c, yx], held.at[c, most], held.at[c, most])
        value = split(held.reshape(3, 512, 128)[c])
        both = jnp.concatenate(value, axis=1)
        top = mm(fx_high[...], both)
        value = top[:, :128] + (top[:, 128:] + mm(fx_low[...], value[0]))
        re, im = value[:256], value[256:]
        cos, sin = turn_cos[...], turn_sin[...]
        turned = jnp.concatenate([re * cos + im * sin, im * cos - re * sin], axis=1)
        high, low = split(turned)
        modes[c] = mm(high, mix[...]) + mm(low, mix[...])

    half_way(0)
    slot_tile = lax.broadcasted_iota(jnp.int32, (start.shape[1] // 128, SLOTS), 0)
    ends = jnp.concatenate([jnp.where(slot_tile == pairs[e : e + 1, :], 1.0, 0.0) for e in range(2)], axis=1)
    pick_tiles(ends, start, fraction, force, by_tile, tiles)
    for copy in table_copies:
        copy.wait()
    bx_high[...] = fx_high[...].T
    bx_low[...] = fx_low[...].T
    near_terms(tiles, terms, 0, 12)
    half_way(1)
    line_modes(0)
    back_modes(start, fraction, (bz_high[...], bz_low[...]), z_own)
    back_modes(start_b, fraction_b, (bz_high[...], bz_low[...]), z_behind)
    near_terms(tiles, terms, 12, 16)
    half_way(2)
    line_modes(1)
    line_modes(2)

    column = zc * 16 + yx
    lane = lax.broadcasted_iota(jnp.int32, (256, 128), 1)
    row = lax.broadcasted_iota(jnp.int32, (256, 128), 0)
    index_x = row + 256 * (lane >> 5)
    index_y = (lane & 31) + 32 * (column >> 6)
    index_z = column & 63
    step_x = TWO_PI / NX
    step_y = TWO_PI / NY
    wave_x = jnp.where(index_x > 512, index_x - 1024, index_x).astype(F32) * step_x
    wave_y = jnp.where(index_y > 64, index_y - 128, index_y).astype(F32) * step_y
    wave_z = index_z.astype(F32) * step_y
    squared = wave_x * wave_x + wave_y * wave_y + wave_z * wave_z
    anchor = squared == 0.0
    drop = anchor | (index_x == 512) | (index_y == 64)
    inverse = jnp.where(drop, 0.0, 1.0 / jnp.where(anchor, 1.0, squared))
    waves = (wave_x, wave_y, wave_z)
    for part in range(2):
        lanes = slice(part * 128, part * 128 + 128)
        values = [modes[c, :, lanes] for c in range(3)]
        project = (wave_x * values[0] + wave_y * values[1] + wave_z * values[2]) * inverse
        for c in range(3):
            modes[c, :, lanes] = (values[c] - waves[c] * project) * inverse

    def way_back(c):
        high, low = split(modes[c])
        value = mm(high, unmix[...]) + mm(low, unmix[...])
        re, im = value[:, :128], value[:, 128:]
        cos, sin = turn_cos[...], turn_sin[...]
        value = split(jnp.concatenate([re * cos - im * sin, im * cos + re * sin], axis=0))
        both = jnp.concatenate(value, axis=1)
        top = mm(bx_high[...], both)
        back[c] = top[:, :128] + (top[:, 128:] + mm(bx_low[...], value[0]))
        phase(2, c, lambda y: back_blocks.at[c, y], mid_b.at[c, yx], False)

    def last_way(c):
        finish(2, c, back_blocks.at[c, yx], mid_b.at[c, yx], back_blocks.at[c, most], mid_b.at[c, most])
        phase(3, c, lambda z: mid_b.at[c, :, z], lines_blocks.at[c, zc], True)

    way_back(0)
    way_back(1)
    way_back(2)
    near_terms(tiles, terms, 16, 22)
    last_way(0)
    near_terms(tiles, terms, 22, 30)
    last_way(1)
    near_terms(tiles, terms, 30, 38)
    last_way(2)
    near_terms(tiles, terms, 38, SLOTS)
    slot = lax.broadcasted_iota(jnp.int32, slot_tile.shape, 1)
    live = jnp.where((slot_tile == pairs[0:1, :]) & (slot < used[0]), 1.0, 0.0)
    near_sum(live, terms, near)

    last = pltpu.make_async_remote_copy(
        src_ref=partial,
        dst_ref=partial_in,
        send_sem=last_send,
        recv_sem=last_recv,
        device_id=near_by(255),
        device_id_type=MESH,
    )
    for c in range(3):
        finish(3, c, mid_b.at[c, :, zc], lines_blocks.at[c, zc], lines_blocks.at[c, most], lines_blocks.at[c, most])
        lines_back(lines, c, table_y, left)
        gather(c, 3, y_behind, z_behind, a_behind, left, partial)
        if c == 2:
            last.start()
        gather(c, 4, y_own, z_own, a_own, left, out)
    last.wait()
    out[...] = out[...] + near[...]


def step(forces, stencil_start, fraction, tile_pairs, pair_count, tables):
    count = forces.shape[1]
    vmem = pl.BlockSpec(memory_space=pltpu.VMEM)
    far = pl.BlockSpec(memory_space=pl.ANY)
    blocks = (3, 16, 16, 2, 128)
    x_tables = [*tables["forward_x"], tables["mix"], tables["unmix"], *tables["turn"]]
    dma = pltpu.SemaphoreType.DMA
    return pl.pallas_call(
        step_kernel,
        in_specs=[vmem] * 4 + [pl.BlockSpec(memory_space=pltpu.SMEM)] + [vmem] * 6 + [far] * 6,
        out_specs=[vmem, vmem],
        out_shape=[jax.ShapeDtypeStruct((3, count), F32)] * 2,
        scratch_shapes=[
            VMEM((3, count), jnp.int32),
            VMEM((3, count), F32),
            VMEM((3, count), F32),
            VMEM((2, 256, count), BF16),
            VMEM((2, 128, count), F32),
            VMEM((2, 8, count), F32),
            VMEM((3, 512, 256), F32),
            VMEM((3, 512, 256), BF16),
            VMEM((count // 128, 16, 128), F32),
            VMEM((2 * SLOTS, 16, 128), F32),
            VMEM((3, SLOTS, 128), F32),
            VMEM((3, count), F32),
        ]
        + [VMEM(t.shape, t.dtype) for t in x_tables]
        + [VMEM((512, 512), BF16)] * 2
        + [
            VMEM((3, 512, 128), F32),
            VMEM(blocks, F32),
            VMEM(blocks, F32),
            VMEM((3, 512, 128), F32),
            VMEM(blocks, F32),
            VMEM((3, 512, 128), F32),
            VMEM((3, 256, 256), F32),
            VMEM((3, count), F32),
            dma((4, 3)),
            dma((4, 3)),
            dma((4, 3)),
            dma((6,)),
            dma((3,)),
            dma((3,)),
            dma,
            dma,
        ],
        compiler_params=pltpu.CompilerParams(collective_id=0, has_side_effects=True),
        name="step",
    )(
        stencil_start,
        fraction,
        forces,
        tile_pairs.T,
        pair_count,
        *tables["forward_z"],
        *tables["back_z"],
        *tables["table_y"],
        *x_tables,
    )


def per_device(tables, forces, stencil_start, fraction, tile_pairs, pair_count):
    far, behind = step(forces, stencil_start, fraction, tile_pairs, pair_count, tables)
    return far + behind


def solution(mesh):
    tables = make_tables()
    in_specs = (
        P(None, ("group", "dev")),
        P(None, ("group", "dev")),
        P(None, ("group", "dev")),
        P(("group", "dev"), None),
        P(("group", "dev")),
    )
    return jax.shard_map(
        functools.partial(per_device, tables),
        mesh=mesh,
        in_specs=in_specs,
        out_specs=P(None, ("group", "dev")),
        check_vma=False,
    )
```
